512 devices in a mesh: expert: 64 (over z_lo, y, x), shard: 8 (over z_hi, core).
Axes of the slice: x: 4, y: 8, z: 8 (z_hi: 4, z_lo: 2; z = z_hi * 2 + z_lo), core: 2. Of those that a mesh axis runs over, the one named last changes fastest.
Arguments:
- w_gate: float32 [64, 2048, 1024], P('expert', 'shard'), may hold values from -0.125 to 0.125
- avg_gate: float32 [64, 2048, 1024], P('expert', 'shard'), may hold values from -0.125 to 0.125
- w_up: float32 [64, 2048, 1024], P('expert', 'shard'), may hold values from -0.125 to 0.125
- avg_up: float32 [64, 2048, 1024], P('expert', 'shard'), may hold values from -0.125 to 0.125
- mix_share: float32 [64], P('expert'), may hold values from 0.2 to 0.8
- router_weight: float32 [2048, 64], P('shard', 'expert'), may hold values from -0.125 to 0.125
- router_gain: float32 [2048], P('shard'), may hold values from 0.25 to 1.75
Outputs:
- serve_gate: bfloat16 [64, 1024, 2048], P('expert')
- serve_up: bfloat16 [64, 1024, 2048], P('expert')
- serve_router: bfloat16 [2048, 64], replicated
The draws below stay inside these ranges and needn't reach their ends.
All inputs are finite; a program needn't handle non-finite values.
Results may differ from the reference program's by a relative error of at most 0.001.
Values may be sent and summed in bfloat16 or wider, within the bound.
A program may use at most 64 MiB of HBM per device.

```python
import jax
import jax.numpy as jnp

EXPERTS = 64
D_MODEL = 2048
D_EXPERT = 1024


def levels(own_key, dims, pieces, low, top_value):
    level, own = 1.0, jax.random.fold_in(own_key, 6)
    for position, parts in pieces:
        draws = jnp.exp(jax.random.uniform(jax.random.fold_in(own, position), (parts,), jnp.float32, low / len(pieces), top_value / len(pieces)))
        level = level * jnp.repeat(draws, dims[position] // parts).reshape([-1 if axis == position else 1 for axis in range(len(dims))])
    return level


def gaussian(key, extent, scale, most, cuts=(), kind=jnp.bfloat16):
    level = levels(key, extent, cuts, -0.22, 0.18) if cuts else 1.0
    values = jax.random.normal(key, extent, jnp.float32) * scale * level
    return jnp.minimum(jnp.maximum(values, -most), most).astype(kind)


def setup_inputs(seed: int = 0) -> dict:
    streams_of = jax.random.split(jax.random.key(seed), 8)
    return {
        "w_gate": gaussian(streams_of[0], (EXPERTS, D_MODEL, D_EXPERT), D_MODEL ** -0.5, 0.125, ((0, 64), (1, 8)), jnp.float32),
        "avg_gate": gaussian(streams_of[1], (EXPERTS, D_MODEL, D_EXPERT), D_MODEL ** -0.5, 0.125, ((0, 64), (1, 8)), jnp.float32),
        "w_up": gaussian(streams_of[2], (EXPERTS, D_MODEL, D_EXPERT), D_MODEL ** -0.5, 0.125, ((0, 64), (1, 8)), jnp.float32),
        "avg_up": gaussian(streams_of[3], (EXPERTS, D_MODEL, D_EXPERT), D_MODEL ** -0.5, 0.125, ((0, 64), (1, 8)), jnp.float32),
        "mix_share": jnp.clip(0.2 + 0.6 * jax.random.uniform(streams_of[4], (EXPERTS,), jnp.float32) ** levels(streams_of[4], (EXPERTS,), ((0, 64),), -0.2, 0.2), 0.2, 0.8),
        "router_weight": gaussian(streams_of[5], (D_MODEL, EXPERTS), D_MODEL ** -0.5, 0.125, ((0, 8), (1, 64)), jnp.float32),
        "router_gain": jnp.clip(1.0 + 0.15 * jax.random.normal(streams_of[6], (D_MODEL,), jnp.float32), 0.25, 1.75),
    }


def reference(w_gate, avg_gate, w_up, avg_up, mix_share, router_weight, router_gain):
    fresh_gate = mix_share[:, None, None] * w_gate + (1.0 - mix_share[:, None, None]) * avg_gate
    fresh_up = mix_share[:, None, None] * w_up + (1.0 - mix_share[:, None, None]) * avg_up
    serve_gate = fresh_gate.astype(jnp.bfloat16)
    serve_gate = jnp.transpose(serve_gate, (0, 2, 1))
    serve_up = fresh_up.astype(jnp.bfloat16)
    serve_up = jnp.transpose(serve_up, (0, 2, 1))
    serve_router = (router_weight * router_gain[:, None]).astype(jnp.bfloat16)
    return serve_gate, serve_up, serve_router
```

```python
import jax
import jax.numpy as jnp
from jax import lax
from jax.experimental import pallas as pl
from jax.experimental.pallas import tpu as pltpu
from jax.sharding import PartitionSpec as P

MESH = pl.DeviceIdType.MESH
D_MODEL, D_EXPERT, EXPERTS, SHARDS = 2048, 1024, 64, 8
WIDE = D_MODEL // SHARDS
ROWS = 128
CHUNKS = D_EXPERT // ROWS
X, Y, Z = 4, 8, 8
EARLY = 4
PARTS = 4


def kernel(wg, ag, wu, au, rw_any, gain_any, mix, gate, up, router, held, held_sem, rw, gain, small_sem, ring, flat,
           ici_send, ici_recv, core_send, core_recv, r_send, r_recv):
    e, s = lax.axis_index("expert"), lax.axis_index("shard")
    z_lo, y, x = e // (Y * X), (e // X) % Y, e % X
    z_hi, c = s // 2, s % 2
    z = 2 * z_hi + z_lo

    def at(x_, y_, z_, c_):
        return {"expert": (z_ % 2) * (Y * X) + y_ * X + x_, "shard": (z_ // 2) * 2 + c_}

    fore, back = at(x, y, (z + 2) % Z, c), at(x, y, (z + Z - 2) % Z, c)
    mate = at(x, y, z, 1 - c)
    steps = {
        "z": (at(x, y, (z + 1) % Z, c), at(x, y, (z + Z - 1) % Z, c)),
        "x": (at((x + 1) % X, y, z, c), at((x + X - 1) % X, y, z, c)),
        "y": (at(x, (y + 1) % Y, z, c), at(x, (y + Y - 1) % Y, z, c)),
    }

    def loads(j):
        cols = pl.ds(pl.multiple_of(j * ROWS, ROWS), ROWS)
        return [pltpu.make_async_copy(ref.at[0, :, cols], held.at[i, :, cols], held_sem.at[i, j])
                for i, ref in enumerate((wg, ag, wu, au))]

    small = [pltpu.make_async_copy(a, b, small_sem.at[i])
             for i, (a, b) in enumerate(((rw_any, rw), (gain_any, gain)))]
    for j in range(CHUNKS):
        for copy in loads(j):
            copy.start()
    small[0].start()
    small[1].start()

    barrier = pltpu.get_barrier_semaphore()
    peers = [fore, back, mate, *steps["z"], *steps["x"], *steps["y"]]
    for peer in peers:
        pl.semaphore_signal(barrier, inc=1, device_id=peer, device_id_type=MESH)

    share = mix[...]
    rest = 1.0 - share

    def columns(shard):
        return pl.ds(pl.multiple_of(shard * WIDE, WIDE), WIDE)

    def compute(j):
        cols = pl.ds(pl.multiple_of(j * ROWS, ROWS), ROWS)
        for copy in loads(j):
            copy.wait()
        for k, out in enumerate((gate, up)):
            fresh = share * held[2 * k, :, cols] + rest * held[2 * k + 1, :, cols]
            out[cols, columns(s)] = fresh.T.astype(jnp.bfloat16)

    def block(out, shard, j):
        return out.at[pl.ds(pl.multiple_of(j * ROWS, ROWS), ROWS), columns(shard)]

    def copy(out, shard, j, to, send, recv):
        ref = block(out, shard, j)
        return pltpu.make_async_remote_copy(ref, ref, send, recv, device_id=to, device_id_type=MESH)

    def hop(lane, kind, j, shard):
        out = (gate, up)[(kind + lane) % 2] if kind < 2 else (gate, up)[lane]
        return copy(out, shard, j, (fore, back)[lane], ici_send.at[lane, kind, j], ici_recv.at[lane, kind, j])

    def across(lane, kind, j, shard):
        if lane == 2:
            out = (gate, up)[kind]
        else:
            out = (gate, up)[(kind + lane) % 2] if kind < 2 else (gate, up)[lane]
        return copy(out, shard, j, mate, core_send.at[lane, kind, j], core_recv.at[lane, kind, j])

    def from_(lane, kind, z_step=0):
        far = 2 if kind == 2 else 1
        d = (4 - far if lane == 0 else far)
        return 2 * ((z_hi + d) % 4)

    def post(i, ref, to):
        return pltpu.make_async_remote_copy(
            ref, ref, r_send.at[i], r_recv.at[i], device_id=to, device_id_type=MESH)

    def piece(k):
        return ring.at[c, y, x, (z + k + Z) % Z]

    def row(k):
        return ring.at[c, y, (x + k + X) % X]

    def plane(k):
        return ring.at[c, (y + k + Y) % Y]

    zp, zm = steps["z"]
    xp, xm = steps["x"]
    yp, ym = steps["y"]
    posts = [
        (piece(0), zp, piece(-1)), (piece(0), zm, piece(1)), (piece(0), fore, piece(-2)), (piece(0), back, piece(2)),
        (piece(-2), zp, piece(-3)), (piece(2), zm, piece(3)), (piece(-2), fore, piece(-4)),
        (row(0), xp, row(-1)), (row(0), xm, row(1)), (row(-1), xp, row(-2)),
        (plane(0), yp, plane(-1)), (plane(0), ym, plane(1)), (plane(-1), yp, plane(-2)), (plane(1), ym, plane(2)),
        (plane(-2), yp, plane(-3)), (plane(2), ym, plane(3)), (plane(-3), yp, plane(-4)),
        (ring.at[c], mate, ring.at[1 - c]),
    ]
    rounds = [
        ((), (0, 1, 2, 3)), ((2, 3), (4, 5, 6)), ((0, 1, 4, 5, 6), (7, 8)), ((7,), (9,)), ((8, 9), (10, 11)),
        ((10, 11), (12, 13)), ((12, 13), (14, 15)), ((14,), (16,)), ((15, 16), (17,)), ((17,), ()),
    ]

    def turn(n):
        waits, sends = rounds[n]
        for i in waits:
            post(i, posts[i][2], posts[i][1]).wait_recv()
        for i in sends:
            post(i, posts[i][0], posts[i][1]).start()

    compute(0)
    small[0].wait()
    small[1].wait()
    ring[c, y, x, z] = rw[...] * gain[...]
    compute(1)
    pl.semaphore_wait(barrier, len(peers))
    turn(0)

    def begin(j):
        for lane in range(2):
            hop(lane, 0, j, s).start()
            across(2, lane, j, s).start()

    begin(0)
    for j in range(2, CHUNKS):
        compute(j)
        begin(j - 1)
        if j == EARLY:
            turn(1)
    begin(CHUNKS - 1)

    def second(j, _):
        for lane in range(2):
            hop(lane, 1, j, s).start()
        return 0

    lax.fori_loop(0, CHUNKS, second, 0)

    for j in range(CHUNKS):
        for lane in range(2):
            shard = from_(lane, 0) + c
            hop(lane, 0, j, shard).wait_recv()
            hop(lane, 2, j, shard).start()
            across(lane, 0, j, shard).start()
        if j + 2 < len(rounds):
            turn(j + 2)

    def lay(i, _):
        yy, xx = i // X, i % X
        for zz in range(Z):
            for cc in range(2):
                lo = (2 * (zz // 2) + cc) * WIDE
                flat[pl.ds((zz % 2) * (Y * X) + i, 1), lo : lo + WIDE] = ring[cc, yy, xx, zz]
        return 0

    lax.fori_loop(0, Y * X, lay, 0)
    router[...] = flat[...].astype(jnp.bfloat16)

    for kind in (1, 2):
        def across_only(j, _):
            for lane in range(2):
                shard = from_(lane, kind) + c
                hop(lane, kind, j, shard).wait_recv()
                across(lane, kind, j, shard).start()
            return 0

        lax.fori_loop(0, CHUNKS, across_only, 0)

    def finish(j, _):
        for lane in range(2):
            for kind in range(3):
                hop(lane, kind, j, s).wait_send()
                across(lane, kind, j, s).wait_send()
                across(lane, kind, j, from_(lane, kind) + 1 - c).wait_recv()
        for kind in range(2):
            across(2, kind, j, s).wait_send()
            across(2, kind, j, 2 * z_hi + 1 - c).wait_recv()
        return 0

    lax.fori_loop(0, CHUNKS, finish, 0)
    for i, (sent, to, _) in enumerate(posts):
        post(i, sent, to).wait_send()


def store(gate, up, router, gate_out, up_out, router_out, sem):
    copies = []
    for k, (a, b) in enumerate(((gate, gate_out), (up, up_out))):
        for i in range(PARTS):
            rows = pl.ds(i * (D_EXPERT // PARTS), D_EXPERT // PARTS)
            copies.append(pltpu.make_async_copy(a.at[rows], b.at[rows], sem.at[k, i]))
    copies.append(pltpu.make_async_copy(router, router_out, sem.at[2, 0]))
    for copy in copies:
        copy.start()
    for copy in copies:
        copy.wait()


def local(w_gate, avg_gate, w_up, avg_up, mix_share, router_weight, router_gain):
    out = jax.ShapeDtypeStruct((D_EXPERT, D_MODEL), jnp.bfloat16)
    hbm = pl.BlockSpec(memory_space=pltpu.HBM)
    vmem = pl.BlockSpec(memory_space=pltpu.VMEM)
    dma = pltpu.SemaphoreType.DMA
    gate, up, router = pl.pallas_call(
        kernel,
        out_shape=(out, out, jax.ShapeDtypeStruct((EXPERTS, D_MODEL), jnp.bfloat16)),
        in_specs=[hbm] * 6 + [vmem],
        out_specs=(vmem, vmem, vmem),
        scratch_shapes=[
            pltpu.VMEM((4, WIDE, D_EXPERT), jnp.float32),
            dma((4, CHUNKS)),
            pltpu.VMEM((1, WIDE), jnp.float32),
            pltpu.VMEM((1, WIDE), jnp.float32),
            dma((2,)),
            pltpu.VMEM((2, Y, X, Z, 1, WIDE), jnp.float32),
            pltpu.VMEM((EXPERTS, D_MODEL), jnp.float32),
            dma((2, 3, CHUNKS)),
            dma((2, 3, CHUNKS)),
            dma((3, 3, CHUNKS)),
            dma((3, 3, CHUNKS)),
            dma((18,)),
            dma((18,)),
        ],
        compiler_params=pltpu.CompilerParams(
            collective_id=0, has_side_effects=True, vmem_limit_bytes=40 * 2**20),
        name="mix_and_gather",
    )(*(pltpu.with_memory_space_constraint(a, pltpu.HBM) for a in (
        w_gate, avg_gate, w_up, avg_up, router_weight.reshape(1, WIDE), router_gain.reshape(1, WIDE))),
        mix_share.reshape(1, 1))
    gate, up, router = pl.pallas_call(
        store,
        out_shape=(out, out, jax.ShapeDtypeStruct((EXPERTS, D_MODEL), jnp.bfloat16)),
        in_specs=[vmem] * 3,
        out_specs=(hbm,) * 3,
        scratch_shapes=[dma((3, PARTS))],
        compiler_params=pltpu.CompilerParams(vmem_limit_bytes=2**20),
        name="store",
    )(gate, up, router)
    return gate[None], up[None], router.T


def solution(mesh):
    return jax.shard_map(
        local,
        mesh=mesh,
        in_specs=(
            P("expert", "shard", None),
            P("expert", "shard", None),
            P("expert", "shard", None),
            P("expert", "shard", None),
            P("expert"),
            P("shard", "expert"),
            P("shard"),
        ),
        out_specs=(P("expert", None, None), P("expert", None, None), P()),
        check_vma=False,
    )
```

```python
import jax
import jax.numpy as jnp
from jax import lax
from jax.experimental import pallas as pl
from jax.experimental.pallas import tpu as pltpu
from jax.sharding import PartitionSpec as P

MESH = pl.DeviceIdType.MESH
D_MODEL, D_EXPERT, EXPERTS, SHARDS = 2048, 1024, 64, 8
WIDE = D_MODEL // SHARDS
ROWS = 128
CHUNKS = D_EXPERT // ROWS
X, Y, Z = 4, 8, 8
FORE, BACK, MATE, ZP, ZM, XP, XM, YP, YM = range(9)
OPPOSITE = (BACK, FORE, MATE, ZM, ZP, XM, XP, YM, YP)
GROUPS = ((0, 1), (1, 3), (4, 4))
OTHER = ((0, 4), (4, 4))
PASSED = ((0, 1), (1, 3), (4, 2), (6, 1), (7, 1))
SHIFT = 0
PARTS = 4


def kernel(wg, ag, wu, au, rw_any, gain_any, mix, gate, up, router, held, load_sem, small, small_sem, ring, flat,
           ready, first_recv, second_recv, passed_recv, ici_send, core_sem, r_send, r_recv):
    e, s = lax.axis_index("expert"), lax.axis_index("shard")
    x, y, z_lo = e & (X - 1), (e >> 2) & (Y - 1), e >> 5
    z_hi, c = s >> 1, s & 1
    z = 2 * z_hi + z_lo

    def columns_of(g):
        return pl.ds(GROUPS[g][0] * ROWS, GROUPS[g][1] * ROWS)

    for i, ref in enumerate((rw_any, gain_any)):
        pltpu.make_async_copy(ref, small.at[i], small_sem).start()
    for g in range(len(GROUPS)):
        for k in (1, 0):
            for i, ref in enumerate(((wg, ag), (wu, au))[k]):
                pltpu.make_async_copy(ref.at[0, :, columns_of(g)], held.at[2 * k + i, :, columns_of(g)], load_sem.at[k, g]).start()

    def loaded(k, g):
        ref = held.at[2 * k : 2 * k + 2, :, columns_of(g)]
        pltpu.make_async_copy(ref, ref, load_sem.at[k, g]).wait()

    def place(dx=0, dy=0, dz=0, dc=0):
        return (x + dx) & (X - 1), (y + dy) & (Y - 1), (z + dz) & (Z - 1), (c + dc) & 1

    def device(p):
        return {"expert": ((p[2] & 1) << 5) + (p[1] << 2) + p[0], "shard": (p[2] & 6) + p[3]}

    def rank(p):
        order = (p[2] << 6) + (p[1] << 3) + (p[0] << 1) + 1 - p[3]
        return jnp.where(order == 1, 2 * X * Y * Z, order)

    places = [place(dz=2), place(dz=-2), place(dc=1), place(dz=1), place(dz=-1), place(dx=1), place(dx=-1), place(dy=1), place(dy=-1)]
    near = [device(p) for p in places]
    own_rank = rank(place())
    earlier = [rank(p) < own_rank for p in places]
    lanes = (FORE, BACK)

    barrier = pltpu.get_barrier_semaphore()
    for k in range(9):
        @pl.when(jnp.logical_not(earlier[k]))
        def _():
            pl.semaphore_signal(barrier, inc=1, device_id=near[k], device_id_type=MESH)
    def answer():
        before = sum(a.astype(jnp.int32) for a in earlier)

        @pl.when(before > 0)
        def _():
            pl.semaphore_wait(barrier, before)

        for k in range(9):
            @pl.when(earlier[k])
            def _():
                pl.semaphore_signal(ready.at[min(OPPOSITE[k], ZP)], inc=1, device_id=near[k], device_id_type=MESH)

    def allow(k):
        @pl.when(jnp.logical_not(earlier[k]))
        def _():
            pl.semaphore_wait(ready.at[k], 1)

    def allow_rest():
        after = sum(1 - earlier[k].astype(jnp.int32) for k in range(ZP, 9))

        @pl.when(after > 0)
        def _():
            pl.semaphore_wait(ready.at[ZP], after)

    share = mix[...]
    rest = 1.0 - share

    def columns(shard):
        return pl.ds(pl.multiple_of(shard * WIDE, WIDE), WIDE)

    def rows(j, n=1):
        return pl.ds(pl.multiple_of(j * ROWS, ROWS), n * ROWS)

    def compute(k, j):
        fresh = share * held[2 * k, :, rows(j)] + rest * held[2 * k + 1, :, rows(j)]
        (gate, up)[k][rows(j), columns(s)] = fresh.T.astype(jnp.bfloat16)

    def copy(k, shard, j, n, to, send, recv):
        ref = (gate, up)[k].at[rows(j, n), columns(shard)]
        return pltpu.make_async_remote_copy(ref, ref, send, recv, device_id=near[to], device_id_type=MESH)

    def first(lane, i, shard):
        return copy(lane, shard, *GROUPS[i], lanes[lane], ici_send.at[lane], first_recv.at[lane, i])

    def second(lane, i, shard):
        return copy(1 - lane, shard, *OTHER[i], lanes[lane], ici_send.at[lane], second_recv.at[i])

    def passed(lane, i, shard, send=2):
        return copy(lane, shard, *PASSED[i], lanes[lane], ici_send.at[send], passed_recv.at[lane, i])

    def across(k, shard, j, n=1):
        return copy(k, shard, j, n, MATE, core_sem.at[0], core_sem.at[1])

    def arriving(lane, far):
        return ((z_hi + (4 - far if lane == 0 else far)) & 3) * 2 + c

    def sent(ref, sem):
        pltpu.make_async_remote_copy(ref, ref, sem, core_sem.at[1], device_id=near[MATE], device_id_type=MESH).wait_send()

    def post(ref, to, i):
        return pltpu.make_async_remote_copy(
            ref, ref, r_send.at[(0, 0, 1, 1, 2, 2, 2, 2, 3)[i]], r_recv.at[i], device_id=near[to], device_id_type=MESH)

    def piece(k):
        return ring.at[c, y, x, (z + k) & (Z - 1)]

    def row(k):
        return ring.at[c, y, (x + k) & (X - 1)]

    def plane(k):
        return ring.at[c, (y + k) & (Y - 1)]

    def landed(ref, i):
        post(ref, MATE, i).wait_recv()

    even = (z & 1) == 0
    zeroth = jnp.logical_or(z < 2, z >= 6)

    def in_turn(order, do):
        for lane in range(2):
            @pl.when(zeroth if lane == order else jnp.logical_not(zeroth))
            def _():
                do(lane)

    def admit(lane):
        allow(lanes[lane])
        post(piece(0), lanes[lane], 0).start()

    def begin(order, *which):
        in_turn(order, lambda lane: [first(lane, i, s).start() for i in which])

    with jax.named_scope("first_chunk"):
        loaded(1, 0)
        compute(1, 0)
        loaded(0, 0)
        compute(0, 0)
        pltpu.make_async_copy(small, small, small_sem).wait()
        ring[c, y, x, z] = small[0] * small[1]
    with jax.named_scope("admit_first"):
        answer()
        in_turn(0, admit)
    with jax.named_scope("compute"):
        def more(j, _):
            for k in (1, 0):
                compute(k, j)
            return 0

        for g in range(1, len(GROUPS)):
            for k in (1, 0):
                loaded(k, g)
            lax.fori_loop(GROUPS[g][0], GROUPS[g][0] + 1, more, 0)

            @pl.when(even)
            def _():
                begin(0, g - 1)

            lax.fori_loop(GROUPS[g][0] + 1, sum(GROUPS[g]), more, 0)
    with jax.named_scope("admit_second"):
        in_turn(1, admit)

        @pl.when(even)
        def _():
            begin(0, 2)
            begin(1, 0, 1)
    with jax.named_scope("z_steps"):
        allow_rest()
        post(piece(0), ZP, 1).start()
        post(piece(0), ZM, 1).start()
        landed(ring.at[c, y, x, 0:2], 0)
        post(piece(-2), ZP, 1).start()
        post(piece(2), ZM, 1).start()
        post(piece(-2), FORE, 1).start()
    with jax.named_scope("own"):
        @pl.when(even)
        def _():
            begin(1, 2)

        @pl.when(jnp.logical_not(even))
        def _():
            begin(0, 0, 1, 2)
            begin(1, 0, 1, 2)

        for i in range(len(OTHER)):
            for lane in range(2):
                second(lane, i, s).start()
    with jax.named_scope("mate_own"):
        allow(MATE)
        for k in range(2):
            across(k, s, 0, CHUNKS).start()

    def own_arrived(i):
        with jax.named_scope(f"half_a{i}"):
            for lane in range(2):
                shard = arriving(lane, 1)
                first(lane, i, shard).wait_recv()
                for p, (lo, n) in enumerate(PASSED):
                    if GROUPS[i][0] <= lo < sum(GROUPS[i]):
                        if lane == 0 and p < SHIFT:
                            @pl.when(z < 6)
                            def _():
                                passed(0, p, shard, 3).start()
                        else:
                            passed(lane, p, shard).start()
                across(lane, shard, *GROUPS[i]).start()

    def other_arrived(i):
        with jax.named_scope(f"half_b{i}"):
            copy(0, s, 0, 2 * OTHER[i][1], MATE, core_sem.at[0], second_recv.at[i]).wait_recv()
            if i < SHIFT:
                @pl.when(jnp.logical_and(z >= 2, z < 4))
                def _():
                    copy(0, arriving(1, 1), *PASSED[0], BACK, ici_send.at[4], passed_recv.at[0, 0]).start()
            for lane in range(2):
                across(1 - lane, arriving(lane, 1), *OTHER[i]).start()

    def router_rest():
        with jax.named_scope("router_x1"):
            landed(ring.at[c, y, x, 0:5], 1)
            post(row(0), XP, 2).start()
            post(row(0), XM, 2).start()
        with jax.named_scope("router_x2"):
            landed(ring.at[c, y, 0:2], 2)
            post(row(-1), XP, 3).start()
        with jax.named_scope("router_y1"):
            landed(ring.at[c, y, 0], 3)
            post(plane(0), YP, 4).start()
            post(plane(0), YM, 4).start()
        for i in range(3):
            with jax.named_scope(f"router_y{i + 2}"):
                landed(ring.at[c, 0:2], 4 + i)
                post(plane(-1 - i), YP, 5 + i).start()
                if i < 2:
                    post(plane(1 + i), YM, 5 + i).start()
        with jax.named_scope("router_mate"):
            landed(ring.at[c, 0], 7)
            post(ring.at[c], MATE, 8).start()

    def arrivals():
        own_arrived(0)
        own_arrived(1)
        other_arrived(0)
        own_arrived(2)
        other_arrived(1)

    @pl.when(even)
    def _():
        arrivals()
        router_rest()

    @pl.when(jnp.logical_not(even))
    def _():
        router_rest()
        arrivals()

    with jax.named_scope("router_end"):
        landed(ring.at[1 - c], 8)

        def lay(i, _):
            yy, xx = i >> 2, i & (X - 1)
            for zz in range(Z):
                for cc in range(2):
                    lo = (2 * (zz // 2) + cc) * WIDE
                    flat[pl.ds((zz % 2) * (Y * X) + i, 1), lo : lo + WIDE] = ring[cc, yy, xx, zz]
            return 0

        lax.fori_loop(0, Y * X, lay, 0)
        router[...] = flat[...].astype(jnp.bfloat16)
    order = [(lane, p) for p in range(len(PASSED)) for lane in range(2)]
    order = order[SHIFT:] + order[:SHIFT]
    for lane, p in order:
        with jax.named_scope(f"passed{p}_{lane}"):
            shard = arriving(lane, 2)
            passed(lane, p, shard).wait_recv()
            across(lane, shard, *PASSED[p]).start()

    with jax.named_scope("finish"):
        sent(gate.at[:, 0 : 2 * WIDE], ici_send.at[0])
        sent(gate.at[:, 0 : 2 * WIDE], ici_send.at[1])
        if SHIFT:
            n = PASSED[0][1] * ROWS
            sent(gate.at[0 : D_EXPERT - n // 2, 0 : 2 * WIDE], ici_send.at[2])
            for i, when in ((3, z < 6), (4, jnp.logical_and(z >= 2, z < 4))):
                @pl.when(when)
                def _():
                    sent(gate.at[0:n, 0:WIDE], ici_send.at[i])
        else:
            sent(gate.at[:, 0 : 2 * WIDE], ici_send.at[2])
        sent(ring.at[c, y, x, 0:7], r_send.at[0])
        sent(ring.at[c, y, 0:3], r_send.at[1])
        sent(ring.at[c, 0:7], r_send.at[2])
        sent(ring.at[c], r_send.at[3])
        sent(gate, core_sem.at[0])
        pltpu.make_async_remote_copy(gate, gate, core_sem.at[0], core_sem.at[1], device_id=near[MATE], device_id_type=MESH).wait_recv()


def store(gate, up, router, gate_out, up_out, router_out, sem):
    copies = []
    for k, (a, b) in enumerate(((gate, gate_out), (up, up_out))):
        for i in range(PARTS):
            rows = pl.ds(i * (D_EXPERT // PARTS), D_EXPERT // PARTS)
            copies.append(pltpu.make_async_copy(a.at[rows], b.at[rows], sem.at[k, i]))
    copies.append(pltpu.make_async_copy(router, router_out, sem.at[2, 0]))
    for copy in copies:
        copy.start()
    for copy in copies:
        copy.wait()


def local(w_gate, avg_gate, w_up, avg_up, mix_share, router_weight, router_gain):
    out = jax.ShapeDtypeStruct((D_EXPERT, D_MODEL), jnp.bfloat16)
    outs = (out, out, jax.ShapeDtypeStruct((EXPERTS, D_MODEL), jnp.bfloat16))
    hbm = pl.BlockSpec(memory_space=pltpu.HBM)
    vmem = pl.BlockSpec(memory_space=pltpu.VMEM)
    dma = pltpu.SemaphoreType.DMA
    gathered = pl.pallas_call(
        kernel,
        out_shape=outs,
        in_specs=[hbm] * 6 + [vmem],
        out_specs=(vmem,) * 3,
        scratch_shapes=[
            pltpu.VMEM((4, WIDE, D_EXPERT), jnp.float32),
            dma((2, len(GROUPS))),
            pltpu.VMEM((2, 1, WIDE), jnp.float32),
            dma,
            pltpu.VMEM((2, Y, X, Z, 1, WIDE), jnp.float32),
            pltpu.VMEM((EXPERTS, D_MODEL), jnp.float32),
            pltpu.SemaphoreType.REGULAR((4,)),
            dma((2, len(GROUPS))),
            dma((len(OTHER),)),
            dma((2, len(PASSED))),
            dma((5,)),
            dma((2,)),
            dma((4,)),
            dma((9,)),
        ],
        compiler_params=pltpu.CompilerParams(
            collective_id=0, has_side_effects=True, vmem_limit_bytes=40 * 2**20),
        name="mix_and_gather",
    )(*(pltpu.with_memory_space_constraint(a, pltpu.HBM) for a in (
        w_gate, avg_gate, w_up, avg_up, router_weight.reshape(1, WIDE), router_gain.reshape(1, WIDE))),
      mix_share.reshape(1, 1))
    gate, up, router = pl.pallas_call(
        store,
        out_shape=outs,
        in_specs=[vmem] * 3,
        out_specs=(hbm,) * 3,
        scratch_shapes=[dma((3, PARTS))],
        compiler_params=pltpu.CompilerParams(vmem_limit_bytes=2**20),
        name="store",
    )(*gathered)
    return gate[None], up[None], router.T


def solution(mesh):
    return jax.shard_map(
        local,
        mesh=mesh,
        in_specs=(
            P("expert", "shard", None),
            P("expert", "shard", None),
            P("expert", "shard", None),
            P("expert", "shard", None),
            P("expert"),
            P("shard", "expert"),
            P("shard"),
        ),
        out_specs=(P("expert", None, None), P("expert", None, None), P()),
        check_vma=False,
    )
```

```python
import jax
import jax.numpy as jnp
from jax import lax
from jax.experimental import pallas as pl
from jax.experimental.pallas import tpu as pltpu
from jax.sharding import PartitionSpec as P

MESH = pl.DeviceIdType.MESH
D_MODEL, D_EXPERT, EXPERTS, SHARDS = 2048, 1024, 64, 8
WIDE = D_MODEL // SHARDS
ROWS = 128
CHUNKS = D_EXPERT // ROWS
X, Y, Z = 4, 8, 8
FORE, BACK, MATE, ZP, ZM, XP, XM, YP, YM = range(9)
OPPOSITE = (BACK, FORE, MATE, ZM, ZP, XM, XP, YM, YP)
GROUPS = ((0, 1), (1, 3), (4, 4))
OTHER = ((0, 2), (2, 6))
PASSED = ((0, 1), (1, 1), (2, 2), (4, 2), (6, 1), (7, 1))
LEFT = (0, 0, 0, 0, 0, 0, 2, 0), (2, 0, 0, 0, 1, 0, 0, 0)
MOST = 2
LATE = 6
PARTS = 4


def kernel(wg, ag, wu, au, rw_any, gain_any, mix, gate, up, router, held, load_sem, small, small_sem, ring, flat,
           ready, first_recv, second_recv, passed_recv, ici_send, core_sem, r_send, r_recv):
    e, s = lax.axis_index("expert"), lax.axis_index("shard")
    x, y, z_lo = e & (X - 1), (e >> 2) & (Y - 1), e >> 5
    z_hi, c = s >> 1, s & 1
    z = 2 * z_hi + z_lo

    def columns_of(g):
        return pl.ds(GROUPS[g][0] * ROWS, GROUPS[g][1] * ROWS)

    for i, ref in enumerate((rw_any, gain_any)):
        pltpu.make_async_copy(ref, small.at[i], small_sem).start()
    for g in range(len(GROUPS)):
        for k in (1, 0):
            for i, ref in enumerate(((wg, ag), (wu, au))[k]):
                pltpu.make_async_copy(ref.at[0, :, columns_of(g)], held.at[2 * k + i, :, columns_of(g)], load_sem.at[k, g]).start()

    def loaded(k, g):
        ref = held.at[2 * k : 2 * k + 2, :, columns_of(g)]
        pltpu.make_async_copy(ref, ref, load_sem.at[k, g]).wait()

    def place(dx=0, dy=0, dz=0, dc=0):
        return (x + dx) & (X - 1), (y + dy) & (Y - 1), (z + dz) & (Z - 1), (c + dc) & 1

    def device(p):
        return {"expert": ((p[2] & 1) << 5) + (p[1] << 2) + p[0], "shard": (p[2] & 6) + p[3]}

    def rank(p):
        order = (p[2] << 7) + (p[1] << 4) + (p[0] << 2) + 2 - 2 * p[3]
        return jnp.where(order == 2, (LATE << 7) - 1, order)

    places = [place(dz=2), place(dz=-2), place(dc=1), place(dz=1), place(dz=-1), place(dx=1), place(dx=-1), place(dy=1), place(dy=-1)]
    near = [device(p) for p in places]
    own_rank = rank(place())
    earlier = [rank(p) < own_rank for p in places]
    lanes = (FORE, BACK)

    barrier = pltpu.get_barrier_semaphore()
    for k in range(9):
        @pl.when(jnp.logical_not(earlier[k]))
        def _():
            pl.semaphore_signal(barrier, inc=1, device_id=near[k], device_id_type=MESH)
    def answer():
        before = sum(a.astype(jnp.int32) for a in earlier)

        @pl.when(before > 0)
        def _():
            pl.semaphore_wait(barrier, before)

        for k in range(9):
            @pl.when(earlier[k])
            def _():
                pl.semaphore_signal(ready.at[min(OPPOSITE[k], ZP)], inc=1, device_id=near[k], device_id_type=MESH)

    def allow(k):
        @pl.when(jnp.logical_not(earlier[k]))
        def _():
            pl.semaphore_wait(ready.at[k], 1)

    def allow_rest():
        after = sum(1 - earlier[k].astype(jnp.int32) for k in range(ZP, 9))

        @pl.when(after > 0)
        def _():
            pl.semaphore_wait(ready.at[ZP], after)

    share = mix[...]
    rest = 1.0 - share

    def columns(shard):
        return pl.ds(pl.multiple_of(shard * WIDE, WIDE), WIDE)

    def rows(j, n=1):
        return pl.ds(pl.multiple_of(j * ROWS, ROWS), n * ROWS)

    def compute(k, j):
        fresh = share * held[2 * k, :, rows(j)] + rest * held[2 * k + 1, :, rows(j)]
        (gate, up)[k][rows(j), columns(s)] = fresh.T.astype(jnp.bfloat16)

    def copy(k, shard, j, n, to, send, recv):
        ref = (gate, up)[k].at[rows(j, n), columns(shard)]
        return pltpu.make_async_remote_copy(ref, ref, send, recv, device_id=near[to], device_id_type=MESH)

    def first(lane, i, shard):
        return copy(lane, shard, *GROUPS[i], lanes[lane], ici_send.at[lane], first_recv.at[lane, i])

    def second(lane, i, shard):
        return copy(1 - lane, shard, *OTHER[i], lanes[lane], ici_send.at[lane], second_recv.at[i])

    def passed(lane, i, shard, send=2):
        return copy(lane, shard, *PASSED[i], lanes[lane], ici_send.at[send], passed_recv.at[lane, i])

    def across(k, shard, j, n=1):
        return copy(k, shard, j, n, MATE, core_sem.at[0], core_sem.at[1])

    def arriving(lane, far):
        return ((z_hi + (4 - far if lane == 0 else far)) & 3) * 2 + c

    def sent(ref, sem):
        pltpu.make_async_remote_copy(ref, ref, sem, core_sem.at[1], device_id=near[MATE], device_id_type=MESH).wait_send()

    def post(ref, to, i):
        return pltpu.make_async_remote_copy(
            ref, ref, r_send.at[(0, 0, 1, 1, 2, 2, 2, 2, 3)[i]], r_recv.at[i], device_id=near[to], device_id_type=MESH)

    def piece(k):
        return ring.at[c, y, x, (z + k) & (Z - 1)]

    def row(k):
        return ring.at[c, y, (x + k) & (X - 1)]

    def plane(k):
        return ring.at[c, (y + k) & (Y - 1)]

    def landed(ref, i):
        post(ref, MATE, i).wait_recv()

    even = (z & 1) == 0
    zeroth = jnp.logical_or(z < 2, z >= 6)

    def in_turn(order, do):
        for lane in range(2):
            @pl.when(zeroth if lane == order else jnp.logical_not(zeroth))
            def _():
                do(lane)

    def own_piece(lane):
        post(piece(0), lanes[lane], 0).start()

    def begin(order, *which):
        in_turn(order, lambda lane: [first(lane, i, s).start() for i in which])

    def begin_other(order, *which):
        in_turn(order, lambda lane: [second(lane, i, s).start() for i in which])

    both = jnp.logical_and(even, z >= 6)
    one = jnp.logical_and(even, z < 6)

    with jax.named_scope("first_chunk"):
        answer()
        loaded(1, 0)
        compute(1, 0)
        loaded(0, 0)
        compute(0, 0)
    with jax.named_scope("admit_first"):
        in_turn(0, lambda lane: allow(lanes[lane]))

        @pl.when(even)
        def _():
            begin(0, 0)

        @pl.when(both)
        def _():
            begin(1, 0)
    with jax.named_scope("compute"):
        def more(j, _):
            for k in (1, 0):
                compute(k, j)
            return 0

        def more_of(g):
            for k in (1, 0):
                loaded(k, g)
            lax.fori_loop(GROUPS[g][0], sum(GROUPS[g]), more, 0)

        more_of(1)
        pltpu.make_async_copy(small, small, small_sem).wait()
        ring[c, y, x, z] = small[0] * small[1]
        in_turn(0, own_piece)

        @pl.when(even)
        def _():
            begin(0, 1)

        @pl.when(both)
        def _():
            in_turn(1, own_piece)
            begin(1, 1)

        @pl.when(even)
        def _():
            begin_other(0, 0)

        more_of(2)
    with jax.named_scope("admit_second"):
        in_turn(1, lambda lane: allow(lanes[lane]))

        @pl.when(jnp.logical_not(both))
        def _():
            in_turn(1, own_piece)

        @pl.when(one)
        def _():
            begin(1, 0, 1)

        @pl.when(even)
        def _():
            begin_other(1, 0)
    with jax.named_scope("z_steps"):
        allow_rest()
        post(piece(0), ZP, 1).start()
        post(piece(0), ZM, 1).start()
        landed(ring.at[c, y, x, 0:2], 0)
        post(piece(-2), ZP, 1).start()
        post(piece(2), ZM, 1).start()
        post(piece(-2), FORE, 1).start()
    with jax.named_scope("own"):
        @pl.when(jnp.logical_not(even))
        def _():
            for order in range(2):
                begin(order, 0, 1)
                begin_other(order, 0)

        for order in range(2):
            begin(order, 2)
            begin_other(order, 1)
    with jax.named_scope("mate_own"):
        allow(MATE)
        for k in range(2):
            across(k, s, 0, CHUNKS).start()

    def on(planes):
        return sum(jnp.where(z == k, 1, 0) for k in planes) > 0

    def direct(lane, p):
        left = [k for k in range(Z) if LEFT[lane][k] > p]
        return jnp.logical_not(on(left)) if left else z >= 0

    def about(lane, p):
        left = [(k + 4) % Z for k in range(Z) if LEFT[lane][k] > p]
        return on(left) if left else z < 0

    def own_arrived(i):
        with jax.named_scope(f"half_a{i}"):
            for lane in range(2):
                shard = arriving(lane, 1)
                first(lane, i, shard).wait_recv()
                for p, (lo, n) in enumerate(PASSED):
                    if GROUPS[i][0] <= lo < sum(GROUPS[i]):
                        if p < MOST:
                            @pl.when(direct(lane, p))
                            def _():
                                passed(lane, p, shard, 3 + MOST * lane + p).start()
                        else:
                            passed(lane, p, shard).start()
                across(lane, shard, *GROUPS[i]).start()

    def other_arrived(i):
        with jax.named_scope(f"half_b{i}"):
            ref = gate.at[rows(0, OTHER[i][1]), 0 : 2 * WIDE]
            pltpu.make_async_remote_copy(ref, ref, core_sem.at[0], second_recv.at[i], device_id=near[MATE], device_id_type=MESH).wait_recv()
            for lane in range(2):
                for p, (lo, n) in enumerate(PASSED[:MOST]):
                    if OTHER[i][0] <= lo < sum(OTHER[i]):
                        @pl.when(about(lane, p))
                        def _():
                            copy(lane, arriving(1 - lane, 1), lo, n, lanes[1 - lane], ici_send.at[3 + 2 * MOST + p], passed_recv.at[lane, p]).start()
            for lane in range(2):
                across(1 - lane, arriving(lane, 1), *OTHER[i]).start()

    def router_rest():
        with jax.named_scope("router_x1"):
            landed(ring.at[c, y, x, 0:5], 1)
            post(row(0), XP, 2).start()
            post(row(0), XM, 2).start()
        with jax.named_scope("router_x2"):
            landed(ring.at[c, y, 0:2], 2)
            post(row(-1), XP, 3).start()
        with jax.named_scope("router_y1"):
            landed(ring.at[c, y, 0], 3)
            post(plane(0), YP, 4).start()
            post(plane(0), YM, 4).start()
        for i in range(3):
            with jax.named_scope(f"router_y{i + 2}"):
                landed(ring.at[c, 0:2], 4 + i)
                post(plane(-1 - i), YP, 5 + i).start()
                if i < 2:
                    post(plane(1 + i), YM, 5 + i).start()
        with jax.named_scope("router_mate"):
            landed(ring.at[c, 0], 7)
            post(ring.at[c], MATE, 8).start()

    def arrivals():
        own_arrived(0)
        own_arrived(1)
        other_arrived(0)
        own_arrived(2)

    @pl.when(even)
    def _():
        arrivals()
        router_rest()
        other_arrived(1)

    @pl.when(jnp.logical_not(even))
    def _():
        router_rest()
        arrivals()
        other_arrived(1)

    with jax.named_scope("router_end"):
        landed(ring.at[1 - c], 8)

        def lay(i, _):
            yy, xx = i >> 2, i & (X - 1)
            for zz in range(Z):
                for cc in range(2):
                    lo = (2 * (zz // 2) + cc) * WIDE
                    flat[pl.ds((zz % 2) * (Y * X) + i, 1), lo : lo + WIDE] = ring[cc, yy, xx, zz]
            return 0

        lax.fori_loop(0, Y * X, lay, 0)
        router[...] = flat[...].astype(jnp.bfloat16)
    order = [(lane, p) for p in range(len(PASSED)) for lane in range(2)]
    order = order[2 * MOST :] + order[: 2 * MOST]
    for lane, p in order:
        with jax.named_scope(f"passed{p}_{lane}"):
            shard = arriving(lane, 2)
            passed(lane, p, shard).wait_recv()
            across(lane, shard, *PASSED[p]).start()

    with jax.named_scope("finish"):
        sent(gate.at[:, 0 : 2 * WIDE], ici_send.at[0])
        sent(gate.at[:, 0 : 2 * WIDE], ici_send.at[1])
        sent(gate.at[0 : D_EXPERT - sum(n for _, n in PASSED[:MOST]) * ROWS, 0 : 2 * WIDE], ici_send.at[2])
        for p, (_, n) in enumerate(PASSED[:MOST]):
            for i, when in (
                (3 + p, direct(0, p)), (3 + MOST + p, direct(1, p)), (3 + 2 * MOST + p, jnp.logical_or(about(0, p), about(1, p)))):
                @pl.when(when)
                def _():
                    sent(gate.at[0 : n * ROWS, 0:WIDE], ici_send.at[i])
        sent(ring.at[c, y, x, 0:7], r_send.at[0])
        sent(ring.at[c, y, 0:3], r_send.at[1])
        sent(ring.at[c, 0:7], r_send.at[2])
        sent(ring.at[c], r_send.at[3])
        sent(gate, core_sem.at[0])
        pltpu.make_async_remote_copy(gate, gate, core_sem.at[0], core_sem.at[1], device_id=near[MATE], device_id_type=MESH).wait_recv()


def store(gate, up, router, gate_out, up_out, router_out, sem):
    copies = []
    for k, (a, b) in enumerate(((gate, gate_out), (up, up_out))):
        for i in range(PARTS):
            rows = pl.ds(i * (D_EXPERT // PARTS), D_EXPERT // PARTS)
            copies.append(pltpu.make_async_copy(a.at[rows], b.at[rows], sem.at[k, i]))
    copies.append(pltpu.make_async_copy(router, router_out, sem.at[2, 0]))
    for copy in copies:
        copy.start()
    for copy in copies:
        copy.wait()


def local(w_gate, avg_gate, w_up, avg_up, mix_share, router_weight, router_gain):
    out = jax.ShapeDtypeStruct((D_EXPERT, D_MODEL), jnp.bfloat16)
    outs = (out, out, jax.ShapeDtypeStruct((EXPERTS, D_MODEL), jnp.bfloat16))
    hbm = pl.BlockSpec(memory_space=pltpu.HBM)
    vmem = pl.BlockSpec(memory_space=pltpu.VMEM)
    dma = pltpu.SemaphoreType.DMA
    gathered = pl.pallas_call(
        kernel,
        out_shape=outs,
        in_specs=[hbm] * 6 + [vmem],
        out_specs=(vmem,) * 3,
        scratch_shapes=[
            pltpu.VMEM((4, WIDE, D_EXPERT), jnp.float32),
            dma((2, len(GROUPS))),
            pltpu.VMEM((2, 1, WIDE), jnp.float32),
            dma,
            pltpu.VMEM((2, Y, X, Z, 1, WIDE), jnp.float32),
            pltpu.VMEM((EXPERTS, D_MODEL), jnp.float32),
            pltpu.SemaphoreType.REGULAR((4,)),
            dma((2, len(GROUPS))),
            dma((len(OTHER),)),
            dma((2, len(PASSED))),
            dma((3 + 3 * MOST,)),
            dma((2,)),
            dma((4,)),
            dma((9,)),
        ],
        compiler_params=pltpu.CompilerParams(
            collective_id=0, has_side_effects=True, vmem_limit_bytes=40 * 2**20),
        name="mix_and_gather",
    )(*(pltpu.with_memory_space_constraint(a, pltpu.HBM) for a in (
        w_gate, avg_gate, w_up, avg_up, router_weight.reshape(1, WIDE), router_gain.reshape(1, WIDE))),
      mix_share.reshape(1, 1))
    gate, up, router = pl.pallas_call(
        store,
        out_shape=outs,
        in_specs=[vmem] * 3,
        out_specs=(hbm,) * 3,
        scratch_shapes=[dma((3, PARTS))],
        compiler_params=pltpu.CompilerParams(vmem_limit_bytes=2**20),
        name="store",
    )(*gathered)
    return gate[None], up[None], router.T


def solution(mesh):
    return jax.shard_map(
        local,
        mesh=mesh,
        in_specs=(
            P("expert", "shard", None),
            P("expert", "shard", None),
            P("expert", "shard", None),
            P("expert", "shard", None),
            P("expert"),
            P("shard", "expert"),
            P("shard"),
        ),
        out_specs=(P("expert", None, None), P("expert", None, None), P()),
        check_vma=False,
    )
```

```python
import jax
import jax.numpy as jnp
from jax import lax
from jax.experimental import pallas as pl
from jax.experimental.pallas import tpu as pltpu
from jax.sharding import PartitionSpec as P

MESH = pl.DeviceIdType.MESH
D_MODEL, D_EXPERT, EXPERTS, SHARDS = 2048, 1024, 64, 8
WIDE = D_MODEL // SHARDS
ROWS = 128
CHUNKS = D_EXPERT // ROWS
X, Y, Z = 4, 8, 8
FORE, BACK, MATE, ZP, ZM, XP, XM, YP, YM, FORE_MATE, BACK_MATE = range(11)
OPPOSITE = (BACK, FORE, MATE, ZM, ZP, XM, XP, YM, YP, BACK_MATE, FORE_MATE)
TWICE = 32
GROUPS = ((0, 1), (1, 3), (4, 4))
OTHER = ((0, 2), (2, 6))
PASSED = ((0, 128), (128, 128), (256, 256), (512, 256), (768, 128), (896, 128 - TWICE), (1024 - TWICE, TWICE))
LEFT = (0, 0, 0, 0, 0, 0, 2, 0), (2, 0, 0, 0, 1, 0, 0, 0)
MOST = 2
LAST = len(PASSED) - 1
LATE = 6


def kernel(wg, ag, wu, au, rw_any, gain_any, mix, gate, up, router, held, load_sem, small, small_sem, ring, flat,
           ready, first_recv, second_recv, passed_recv, ici_send, core_sem, r_send, r_recv):
    e, s = lax.axis_index("expert"), lax.axis_index("shard")
    x, y, z_lo = e & (X - 1), (e >> 2) & (Y - 1), e >> 5
    z_hi, c = s >> 1, s & 1
    z = 2 * z_hi + z_lo

    def columns_of(g):
        return pl.ds(GROUPS[g][0] * ROWS, GROUPS[g][1] * ROWS)

    for i, ref in enumerate((rw_any, gain_any)):
        pltpu.make_async_copy(ref, small.at[i], small_sem).start()
    for g in range(len(GROUPS)):
        for k in (1, 0):
            for i, ref in enumerate(((wg, ag), (wu, au))[k]):
                pltpu.make_async_copy(ref.at[0, :, columns_of(g)], held.at[2 * k + i, :, columns_of(g)], load_sem.at[g]).start()

    def loaded(g):
        ref = held.at[:, :, columns_of(g)]
        pltpu.make_async_copy(ref, ref, load_sem.at[g]).wait()

    def place(dx=0, dy=0, dz=0, dc=0):
        return (x + dx) & (X - 1), (y + dy) & (Y - 1), (z + dz) & (Z - 1), (c + dc) & 1

    def device(p):
        return {"expert": ((p[2] & 1) << 5) + (p[1] << 2) + p[0], "shard": (p[2] & 6) + p[3]}

    def rank(p):
        order = (p[2] << 7) + (p[1] << 4) + (p[0] << 2) + 2 - 2 * p[3]
        return jnp.where(order == 2, (LATE << 7) - 1, order)

    places = [place(dz=2), place(dz=-2), place(dc=1), place(dz=1), place(dz=-1), place(dx=1), place(dx=-1), place(dy=1), place(dy=-1),
              place(dz=2, dc=1), place(dz=-2, dc=1)]
    near = [device(p) for p in places]
    own_rank = rank(place())
    earlier = [rank(p) < own_rank for p in places]
    lanes = (FORE, BACK)

    barrier = pltpu.get_barrier_semaphore()
    for k in range(11):
        @pl.when(jnp.logical_not(earlier[k]))
        def _():
            pl.semaphore_signal(barrier, inc=1, device_id=near[k], device_id_type=MESH)
    def answer():
        before = sum(a.astype(jnp.int32) for a in earlier)

        @pl.when(before > 0)
        def _():
            pl.semaphore_wait(barrier, before)

        for k in range(11):
            @pl.when(earlier[k])
            def _():
                pl.semaphore_signal(ready.at[min(OPPOSITE[k], ZP)], inc=1, device_id=near[k], device_id_type=MESH)

    def allow(k):
        @pl.when(jnp.logical_not(earlier[k]))
        def _():
            pl.semaphore_wait(ready.at[k], 1)

    def allow_rest():
        after = sum(1 - earlier[k].astype(jnp.int32) for k in range(ZP, 11))

        @pl.when(after > 0)
        def _():
            pl.semaphore_wait(ready.at[ZP], after)

    share = mix[...]
    rest = 1.0 - share

    def columns(shard):
        return pl.ds(pl.multiple_of(shard * WIDE, WIDE), WIDE)

    def rows(j, n=1):
        return pl.ds(pl.multiple_of(j * ROWS, ROWS), n * ROWS)

    def compute(k, j):
        fresh = share * held[2 * k, :, rows(j)] + rest * held[2 * k + 1, :, rows(j)]
        (gate, up)[k][rows(j), columns(s)] = fresh.T.astype(jnp.bfloat16)

    def copy(k, shard, lo, n, to, send, recv):
        ref = (gate, up)[k].at[pl.ds(lo, n), columns(shard)]
        return pltpu.make_async_remote_copy(ref, ref, send, recv, device_id=near[to], device_id_type=MESH)

    def chunks(j, n):
        return j * ROWS, n * ROWS

    def first(lane, i):
        return copy(lane, s, *chunks(*GROUPS[i]), lanes[lane], ici_send.at[0], first_recv.at[i])

    def second(lane, i):
        return copy(1 - lane, s, *chunks(*OTHER[i]), lanes[lane], ici_send.at[0], second_recv.at[i])

    def passed(lane, p, shard, send=0):
        return copy(lane, shard, *PASSED[p], lanes[lane], ici_send.at[send], passed_recv.at[p])

    def across(k, shard, lo, n):
        return copy(k, shard, lo, n, MATE, core_sem.at[0], core_sem.at[1])

    def arrived(n, sem):
        ref = gate.at[0:n, 0 : 2 * WIDE]
        pltpu.make_async_remote_copy(ref, ref, core_sem.at[0], sem, device_id=near[MATE], device_id_type=MESH).wait_recv()

    def arriving(lane, far):
        return ((z_hi + (4 - far if lane == 0 else far)) & 3) * 2 + c

    def sent(ref, sem):
        pltpu.make_async_remote_copy(ref, ref, sem, core_sem.at[1], device_id=near[MATE], device_id_type=MESH).wait_send()

    def post(ref, to, i):
        return pltpu.make_async_remote_copy(
            ref, ref, r_send.at[min(i // 2, 1)], r_recv.at[i], device_id=near[to], device_id_type=MESH)

    def piece(k):
        return ring.at[c, y, x, (z + k) & (Z - 1)]

    def row(k):
        return ring.at[c, y, (x + k) & (X - 1)]

    def plane(k):
        return ring.at[c, (y + k) & (Y - 1)]

    def landed(ref, i):
        post(ref, MATE, i).wait_recv()

    even = (z & 1) == 0
    zeroth = jnp.logical_or(z < 2, z >= 6)

    def in_turn(order, do):
        for lane in range(2):
            @pl.when(zeroth if lane == order else jnp.logical_not(zeroth))
            def _():
                do(lane)

    def own_piece(lane):
        post(piece(0), lanes[lane], 0).start()

    def begin(order, *which):
        in_turn(order, lambda lane: [first(lane, i).start() for i in which])

    def begin_other(order, *which):
        in_turn(order, lambda lane: [second(lane, i).start() for i in which])

    both = jnp.logical_and(even, z >= 6)
    one = jnp.logical_and(even, z < 6)

    with jax.named_scope("first_chunk"):
        answer()
        loaded(0)
        compute(1, 0)
        compute(0, 0)
    with jax.named_scope("admit_first"):
        in_turn(0, lambda lane: allow(lanes[lane]))

        @pl.when(even)
        def _():
            begin(0, 0)

        @pl.when(both)
        def _():
            begin(1, 0)
    with jax.named_scope("compute"):
        def more(j, _):
            for k in (1, 0):
                compute(k, j)
            return 0

        def more_of(g):
            loaded(g)
            lax.fori_loop(GROUPS[g][0], sum(GROUPS[g]), more, 0)

        more_of(1)
        pltpu.make_async_copy(small, small, small_sem).wait()
        ring[c, y, x, z] = small[0] * small[1]
        in_turn(0, own_piece)

        @pl.when(even)
        def _():
            begin(0, 1)

        @pl.when(both)
        def _():
            in_turn(1, own_piece)
            begin(1, 1)

        @pl.when(even)
        def _():
            begin_other(0, 0)

        more_of(2)
    with jax.named_scope("admit_second"):
        in_turn(1, lambda lane: allow(lanes[lane]))

        @pl.when(jnp.logical_not(both))
        def _():
            in_turn(1, own_piece)

        @pl.when(one)
        def _():
            begin(1, 0, 1)

        @pl.when(even)
        def _():
            begin_other(1, 0)
    with jax.named_scope("z_steps"):
        allow_rest()
        post(piece(0), ZP, 1).start()
        post(piece(0), ZM, 1).start()
        landed(ring.at[c, y, x, 0:2], 0)
        post(piece(-2), ZP, 1).start()
        post(piece(2), ZM, 1).start()
        post(piece(-2), FORE, 1).start()
    with jax.named_scope("own"):
        @pl.when(jnp.logical_not(even))
        def _():
            for order in range(2):
                begin(order, 0, 1)
                begin_other(order, 0)

        for order in range(2):
            begin(order, 2)
            begin_other(order, 1)
    with jax.named_scope("mate_own"):
        allow(MATE)
        for k in range(2):
            across(k, s, 0, D_EXPERT).start()

    def on(planes):
        return sum(jnp.where(z == k, 1, 0) for k in planes) > 0

    def direct(lane, p):
        left = [k for k in range(Z) if LEFT[lane][k] > p]
        return jnp.logical_not(on(left)) if left else z >= 0

    def about(lane, p):
        left = [(k + 4) % Z for k in range(Z) if LEFT[lane][k] > p]
        return on(left) if left else z < 0

    odd = jnp.logical_not(even)

    def own_arrived(i):
        with jax.named_scope(f"half_a{i}"):
            start, length = chunks(*GROUPS[i])
            arrived(length, first_recv.at[i])
            for lane in range(2):
                shard = arriving(lane, 1)
                for p, (lo, n) in enumerate(PASSED):
                    if start <= lo < start + length:
                        if p < MOST:
                            @pl.when(direct(lane, p))
                            def _():
                                passed(lane, p, shard, 1 + MOST * lane + p).start()
                        else:
                            passed(lane, p, shard).start()
                        if p == LAST:
                            @pl.when(odd)
                            def _():
                                copy(lane, shard, lo, n, (FORE_MATE, BACK_MATE)[lane], ici_send.at[1 + 3 * MOST], passed_recv.at[LAST + 1]).start()
                across(lane, shard, start, length).start()

    def other_arrived(i):
        with jax.named_scope(f"half_b{i}"):
            start, length = chunks(*OTHER[i])
            arrived(length, second_recv.at[i])
            for lane in range(2):
                for p, (lo, n) in enumerate(PASSED[:MOST]):
                    if start <= lo < start + length:
                        @pl.when(about(lane, p))
                        def _():
                            copy(lane, arriving(1 - lane, 1), lo, n, lanes[1 - lane], ici_send.at[1 + 2 * MOST + p], passed_recv.at[p]).start()
            for lane in range(2):
                across(1 - lane, arriving(lane, 1), start, length).start()

    def router_rest():
        with jax.named_scope("router_x1"):
            landed(ring.at[c, y, x, 0:5], 1)
            post(row(0), XP, 2).start()
            post(row(0), XM, 2).start()
        with jax.named_scope("router_x2"):
            landed(ring.at[c, y, 0:2], 2)
            post(row(-1), XP, 3).start()
        with jax.named_scope("router_y1"):
            landed(ring.at[c, y, 0], 3)
            post(plane(0), YP, 4).start()
            post(plane(0), YM, 4).start()
        for i in range(3):
            with jax.named_scope(f"router_y{i + 2}"):
                landed(ring.at[c, 0:2], 4 + i)
                post(plane(-1 - i), YP, 5 + i).start()
                if i < 2:
                    post(plane(1 + i), YM, 5 + i).start()
        with jax.named_scope("router_mate"):
            landed(ring.at[c, 0], 7)
            post(ring.at[c], MATE, 8).start()

    def arrivals():
        own_arrived(0)
        own_arrived(1)
        other_arrived(0)
        own_arrived(2)

    @pl.when(even)
    def _():
        arrivals()
        router_rest()
        other_arrived(1)

    @pl.when(jnp.logical_not(even))
    def _():
        router_rest()
        arrivals()
        other_arrived(1)

    with jax.named_scope("router_end"):
        landed(ring.at[1 - c], 8)

        def lay(i, _):
            yy, xx = i >> 2, i & (X - 1)
            for zz in range(Z):
                for cc in range(2):
                    lo = (2 * (zz // 2) + cc) * WIDE
                    flat[pl.ds((zz % 2) * (Y * X) + i, 1), lo : lo + WIDE] = ring[cc, yy, xx, zz]
            return 0

        lax.fori_loop(0, Y * X, lay, 0)
        router[...] = flat[...].astype(jnp.bfloat16)
    for p, (lo, n) in enumerate(PASSED):
        with jax.named_scope(f"passed{p}"):
            arrived(n, passed_recv.at[p])
            if p < LAST:
                for lane in range(2):
                    across(lane, arriving(lane, 2), lo, n).start()

    with jax.named_scope("finish"):
        @pl.when(even)
        def _():
            for lane in range(2):
                across(lane, arriving(lane, 2), *PASSED[LAST]).start()

        always = 4 * D_EXPERT + 2 * sum(n for _, n in PASSED[MOST:])
        sent(gate.at[0 : always // SHARDS, :], ici_send.at[0])
        for p, (_, n) in enumerate(PASSED[:MOST]):
            for i, when in ((0, direct(0, p)), (1, direct(1, p)), (2, jnp.logical_or(about(0, p), about(1, p)))):
                @pl.when(when)
                def _():
                    sent(gate.at[0:n, 0:WIDE], ici_send.at[1 + MOST * i + p])
        sent(ring.at[c, y, x, 0:7], r_send.at[0])
        sent(held.at[0, 0:168, 0:768], r_send.at[1])

        def swapped(ref):
            sent(ref, core_sem.at[0])
            pltpu.make_async_remote_copy(ref, ref, core_sem.at[0], core_sem.at[1], device_id=near[MATE], device_id_type=MESH).wait_recv()

        @pl.when(odd)
        def _():
            sent(gate.at[0:TWICE, 0 : 2 * WIDE], ici_send.at[1 + 3 * MOST])
            arrived(TWICE, passed_recv.at[LAST + 1])
            swapped(gate.at[0 : D_EXPERT - 2 * TWICE // SHARDS, :])

        @pl.when(even)
        def _():
            swapped(gate)


def store(gate, up, router, gate_out, up_out, router_out, sem):
    copies = [pltpu.make_async_copy(a, b, sem.at[i])
              for i, (a, b) in enumerate(((gate, gate_out), (up, up_out), (router, router_out)))]
    for copy in copies:
        copy.start()
    for copy in copies:
        copy.wait()


def local(w_gate, avg_gate, w_up, avg_up, mix_share, router_weight, router_gain):
    out = jax.ShapeDtypeStruct((D_EXPERT, D_MODEL), jnp.bfloat16)
    outs = (out, out, jax.ShapeDtypeStruct((EXPERTS, D_MODEL), jnp.bfloat16))
    hbm = pl.BlockSpec(memory_space=pltpu.HBM)
    vmem = pl.BlockSpec(memory_space=pltpu.VMEM)
    dma = pltpu.SemaphoreType.DMA
    gathered = pl.pallas_call(
        kernel,
        out_shape=outs,
        in_specs=[hbm] * 6 + [vmem],
        out_specs=(vmem,) * 3,
        scratch_shapes=[
            pltpu.VMEM((4, WIDE, D_EXPERT), jnp.float32),
            dma((len(GROUPS),)),
            pltpu.VMEM((2, 1, WIDE), jnp.float32),
            dma,
            pltpu.VMEM((2, Y, X, Z, 1, WIDE), jnp.float32),
            pltpu.VMEM((EXPERTS, D_MODEL), jnp.float32),
            pltpu.SemaphoreType.REGULAR((4,)),
            dma((len(GROUPS),)),
            dma((len(OTHER),)),
            dma((len(PASSED) + 1,)),
            dma((2 + 3 * MOST,)),
            dma((2,)),
            dma((2,)),
            dma((9,)),
        ],
        compiler_params=pltpu.CompilerParams(
            collective_id=0, has_side_effects=True, vmem_limit_bytes=40 * 2**20),
        name="mix_and_gather",
    )(*(pltpu.with_memory_space_constraint(a, pltpu.HBM) for a in (
        w_gate, avg_gate, w_up, avg_up, router_weight.reshape(1, WIDE), router_gain.reshape(1, WIDE))),
      mix_share.reshape(1, 1))
    gate, up, router = pl.pallas_call(
        store,
        out_shape=outs,
        in_specs=[vmem] * 3,
        out_specs=(hbm,) * 3,
        scratch_shapes=[dma((3,))],
        compiler_params=pltpu.CompilerParams(vmem_limit_bytes=2**20),
        name="store",
    )(*gathered)
    return gate[None], up[None], router.T


def solution(mesh):
    return jax.shard_map(
        local,
        mesh=mesh,
        in_specs=(
            P("expert", "shard", None),
            P("expert", "shard", None),
            P("expert", "shard", None),
            P("expert", "shard", None),
            P("expert"),
            P("shard", "expert"),
            P("shard"),
        ),
        out_specs=(P("expert", None, None), P("expert", None, None), P()),
        check_vma=False,
    )
```

```python
import jax
import jax.numpy as jnp
from jax import lax
from jax.experimental import pallas as pl
from jax.experimental.pallas import tpu as pltpu
from jax.sharding import PartitionSpec as P

MESH = pl.DeviceIdType.MESH
D_MODEL, D_EXPERT, EXPERTS, SHARDS = 2048, 1024, 64, 8
WIDE = D_MODEL // SHARDS
ROWS = 128
CHUNKS = D_EXPERT // ROWS
X, Y, Z = 4, 8, 8
FORE, BACK, MATE, ZP, ZM, XP, XM, YP, YM, FORE_MATE, BACK_MATE = range(11)
OPPOSITE = (BACK, FORE, MATE, ZM, ZP, XM, XP, YM, YP, BACK_MATE, FORE_MATE)
TWICE = 32
GROUPS = ((0, 1), (1, 3), (4, 4))
OTHER = ((0, 2), (2, 6))
STEP, MOST = 64, 4
PASSED = ((MOST * STEP, 256), (512, 256), (768, 128), (896, 128 - TWICE), (1024 - TWICE, TWICE))
LAST = len(PASSED) - 1
LEFT = (0, 0, 0, 0, 0, 0, 4, 0), (3, 0, 0, 0, 2, 1, 0, 0)
LATE = 6


def kernel(wg, ag, wu, au, rw_any, gain_any, mix, gate, up, router, held, load_sem, small, small_sem, ring, flat,
           ready, first_recv, second_recv, passed_recv, ici_send, core_sem, r_send, r_recv):
    e, s = lax.axis_index("expert"), lax.axis_index("shard")
    x, y, z_lo = e & (X - 1), (e >> 2) & (Y - 1), e >> 5
    z_hi, c = s >> 1, s & 1
    z = 2 * z_hi + z_lo

    def columns_of(g):
        return pl.ds(GROUPS[g][0] * ROWS, GROUPS[g][1] * ROWS)

    for i, ref in enumerate((rw_any, gain_any)):
        pltpu.make_async_copy(ref, small.at[i], small_sem).start()
    for g in range(len(GROUPS)):
        for k in (1, 0):
            for i, ref in enumerate(((wg, ag), (wu, au))[k]):
                pltpu.make_async_copy(ref.at[0, :, columns_of(g)], held.at[2 * k + i, :, columns_of(g)], load_sem.at[g]).start()

    def loaded(g):
        ref = held.at[:, :, columns_of(g)]
        pltpu.make_async_copy(ref, ref, load_sem.at[g]).wait()

    def place(dx=0, dy=0, dz=0, dc=0):
        return (x + dx) & (X - 1), (y + dy) & (Y - 1), (z + dz) & (Z - 1), (c + dc) & 1

    def device(p):
        return {"expert": ((p[2] & 1) << 5) + (p[1] << 2) + p[0], "shard": (p[2] & 6) + p[3]}

    def rank(p):
        order = (p[2] << 7) + (p[1] << 4) + (p[0] << 2) + 2 - 2 * p[3]
        return jnp.where(order == 2, (LATE << 7) - 1, order)

    places = [place(dz=2), place(dz=-2), place(dc=1), place(dz=1), place(dz=-1), place(dx=1), place(dx=-1), place(dy=1), place(dy=-1),
              place(dz=2, dc=1), place(dz=-2, dc=1)]
    near = [device(p) for p in places]
    own_rank = rank(place())
    earlier = [rank(p) < own_rank for p in places]
    lanes = (FORE, BACK)

    barrier = pltpu.get_barrier_semaphore()
    for k in range(11):
        @pl.when(jnp.logical_not(earlier[k]))
        def _():
            pl.semaphore_signal(barrier, inc=1, device_id=near[k], device_id_type=MESH)
    def answer():
        before = sum(a.astype(jnp.int32) for a in earlier)

        @pl.when(before > 0)
        def _():
            pl.semaphore_wait(barrier, before)

        for k in range(11):
            @pl.when(earlier[k])
            def _():
                pl.semaphore_signal(ready.at[min(OPPOSITE[k], ZP)], inc=1, device_id=near[k], device_id_type=MESH)

    def allow(k):
        @pl.when(jnp.logical_not(earlier[k]))
        def _():
            pl.semaphore_wait(ready.at[k], 1)

    def allow_rest():
        after = sum(1 - earlier[k].astype(jnp.int32) for k in range(ZP, 11))

        @pl.when(after > 0)
        def _():
            pl.semaphore_wait(ready.at[ZP], after)

    share = mix[...]
    rest = 1.0 - share

    def columns(shard):
        return pl.ds(pl.multiple_of(shard * WIDE, WIDE), WIDE)

    def rows(j, n=1):
        return pl.ds(pl.multiple_of(j * ROWS, ROWS), n * ROWS)

    def compute(k, j):
        fresh = share * held[2 * k, :, rows(j)] + rest * held[2 * k + 1, :, rows(j)]
        (gate, up)[k][rows(j), columns(s)] = fresh.T.astype(jnp.bfloat16)

    def copy(k, shard, lo, n, to, send, recv):
        ref = (gate, up)[k].at[pl.ds(lo, n), columns(shard)]
        return pltpu.make_async_remote_copy(ref, ref, send, recv, device_id=near[to], device_id_type=MESH)

    def chunks(j, n):
        return j * ROWS, n * ROWS

    def first(lane, i):
        return copy(lane, s, *chunks(*GROUPS[i]), lanes[lane], ici_send.at[0], first_recv.at[i])

    def second(lane, i):
        return copy(1 - lane, s, *chunks(*OTHER[i]), lanes[lane], ici_send.at[0], second_recv.at[i])

    def passed(lane, p, shard):
        return copy(lane, shard, *PASSED[p], lanes[lane], ici_send.at[0], passed_recv.at[p])

    def shared(lane, i, shard, to):
        return copy(lane, shard, i * STEP, STEP, to, ici_send.at[1], passed_recv.at[LAST + 2])

    def across(k, shard, lo, n):
        return copy(k, shard, lo, n, MATE, core_sem.at[0], core_sem.at[1])

    def arrived(n, sem):
        ref = gate.at[0:n, 0 : 2 * WIDE]
        pltpu.make_async_remote_copy(ref, ref, core_sem.at[0], sem, device_id=near[MATE], device_id_type=MESH).wait_recv()

    def arriving(lane, far):
        return ((z_hi + (4 - far if lane == 0 else far)) & 3) * 2 + c

    def sent(ref, sem):
        pltpu.make_async_remote_copy(ref, ref, sem, core_sem.at[1], device_id=near[MATE], device_id_type=MESH).wait_send()

    def post(ref, to, i):
        return pltpu.make_async_remote_copy(
            ref, ref, r_send.at[min(i // 2, 1)], r_recv.at[i], device_id=near[to], device_id_type=MESH)

    def piece(k):
        return ring.at[c, y, x, (z + k) & (Z - 1)]

    def row(k):
        return ring.at[c, y, (x + k) & (X - 1)]

    def plane(k):
        return ring.at[c, (y + k) & (Y - 1)]

    def landed(ref, i):
        post(ref, MATE, i).wait_recv()

    even = (z & 1) == 0
    zeroth = jnp.logical_or(z < 2, z >= 6)

    def in_turn(order, do):
        for lane in range(2):
            @pl.when(zeroth if lane == order else jnp.logical_not(zeroth))
            def _():
                do(lane)

    def own_piece(lane):
        post(piece(0), lanes[lane], 0).start()

    def begin(order, *which):
        in_turn(order, lambda lane: [first(lane, i).start() for i in which])

    def begin_other(order, *which):
        in_turn(order, lambda lane: [second(lane, i).start() for i in which])

    both = jnp.logical_and(even, z >= 6)
    one = jnp.logical_and(even, z < 6)

    with jax.named_scope("first_chunk"):
        answer()
        loaded(0)
        compute(1, 0)
        compute(0, 0)
    with jax.named_scope("admit_first"):
        in_turn(0, lambda lane: allow(lanes[lane]))

        @pl.when(even)
        def _():
            begin(0, 0)

        @pl.when(both)
        def _():
            begin(1, 0)
    with jax.named_scope("compute"):
        def more(j, _):
            for k in (1, 0):
                compute(k, j)
            return 0

        def more_of(g):
            loaded(g)
            lax.fori_loop(GROUPS[g][0], sum(GROUPS[g]), more, 0)

        more_of(1)
        pltpu.make_async_copy(small, small, small_sem).wait()
        ring[c, y, x, z] = small[0] * small[1]
        in_turn(0, own_piece)

        @pl.when(even)
        def _():
            begin(0, 1)

        @pl.when(both)
        def _():
            in_turn(1, own_piece)
            begin(1, 1)

        @pl.when(even)
        def _():
            begin_other(0, 0)

        more_of(2)
    with jax.named_scope("admit_second"):
        in_turn(1, lambda lane: allow(lanes[lane]))

        @pl.when(jnp.logical_not(both))
        def _():
            in_turn(1, own_piece)

        @pl.when(one)
        def _():
            begin(1, 0, 1)

        @pl.when(even)
        def _():
            begin_other(1, 0)
    with jax.named_scope("z_steps"):
        allow_rest()
        post(piece(0), ZP, 1).start()
        post(piece(0), ZM, 1).start()
        landed(ring.at[c, y, x, 0:2], 0)
        post(piece(-2), ZP, 1).start()
        post(piece(2), ZM, 1).start()
        post(piece(-2), FORE, 1).start()
    with jax.named_scope("own"):
        @pl.when(jnp.logical_not(even))
        def _():
            for order in range(2):
                begin(order, 0, 1)
                begin_other(order, 0)

        for order in range(2):
            begin(order, 2)
            begin_other(order, 1)
    with jax.named_scope("mate_own"):
        allow(MATE)
        for k in range(2):
            across(k, s, 0, D_EXPERT).start()

    def at_plane(table):
        return sum(jnp.where(z == k, v, 0) for k, v in enumerate(table) if v) + jnp.where(z < 0, 1, 0)

    left = [at_plane(LEFT[lane]) for lane in range(2)]
    taken = [at_plane([LEFT[lane][(k + 4) % Z] for k in range(Z)]) for lane in range(2)]

    odd = jnp.logical_not(even)

    def own_arrived(i):
        with jax.named_scope(f"half_a{i}"):
            start, length = chunks(*GROUPS[i])
            arrived(length, first_recv.at[i])
            for lane in range(2):
                shard = arriving(lane, 1)
                for j in range(MOST):
                    if start <= j * STEP < start + length:
                        @pl.when(j >= left[lane])
                        def _():
                            shared(lane, j, shard, lanes[lane]).start()
                for p, (lo, n) in enumerate(PASSED):
                    if start <= lo < start + length:
                        passed(lane, p, shard).start()
                        if p == LAST:
                            @pl.when(odd)
                            def _():
                                copy(lane, shard, lo, n, (FORE_MATE, BACK_MATE)[lane], ici_send.at[2], passed_recv.at[LAST + 1]).start()
                across(lane, shard, start, length).start()

    def other_arrived(i):
        with jax.named_scope(f"half_b{i}"):
            start, length = chunks(*OTHER[i])
            arrived(length, second_recv.at[i])
            for lane in range(2):
                for j in range(MOST):
                    if start <= j * STEP < start + length and max(LEFT[lane]) > j:
                        @pl.when(j < taken[lane])
                        def _():
                            shared(lane, j, arriving(1 - lane, 1), lanes[1 - lane]).start()
            for lane in range(2):
                across(1 - lane, arriving(lane, 1), start, length).start()

    def router_rest():
        with jax.named_scope("router_x1"):
            landed(ring.at[c, y, x, 0:5], 1)
            post(row(0), XP, 2).start()
            post(row(0), XM, 2).start()
        with jax.named_scope("router_x2"):
            landed(ring.at[c, y, 0:2], 2)
            post(row(-1), XP, 3).start()
        with jax.named_scope("router_y1"):
            landed(ring.at[c, y, 0], 3)
            post(plane(0), YP, 4).start()
            post(plane(0), YM, 4).start()
        for i in range(3):
            with jax.named_scope(f"router_y{i + 2}"):
                landed(ring.at[c, 0:2], 4 + i)
                post(plane(-1 - i), YP, 5 + i).start()
                if i < 2:
                    post(plane(1 + i), YM, 5 + i).start()
        with jax.named_scope("router_mate"):
            landed(ring.at[c, 0], 7)
            post(ring.at[c], MATE, 8).start()

    def arrivals():
        own_arrived(0)
        own_arrived(1)
        other_arrived(0)
        own_arrived(2)

    @pl.when(even)
    def _():
        arrivals()
        router_rest()
        other_arrived(1)

    @pl.when(jnp.logical_not(even))
    def _():
        router_rest()
        arrivals()
        other_arrived(1)

    with jax.named_scope("router_end"):
        landed(ring.at[1 - c], 8)

        def lay(i, _):
            yy, xx = i >> 2, i & (X - 1)
            for zz in range(Z):
                for cc in range(2):
                    lo = (2 * (zz // 2) + cc) * WIDE
                    flat[pl.ds((zz % 2) * (Y * X) + i, 1), lo : lo + WIDE] = ring[cc, yy, xx, zz]
            return 0

        lax.fori_loop(0, Y * X, lay, 0)
        router[...] = flat[...].astype(jnp.bfloat16)
    def passed_across(lo, n):
        for lane in range(2):
            across(lane, arriving(lane, 2), lo, n).start()

    with jax.named_scope("shared"):
        arrived(MOST * STEP, passed_recv.at[LAST + 2])
        passed_across(0, MOST * STEP)
    for p, (lo, n) in enumerate(PASSED):
        with jax.named_scope(f"passed{p}"):
            arrived(n, passed_recv.at[p])
            if p < LAST:
                passed_across(lo, n)

    with jax.named_scope("finish"):
        @pl.when(even)
        def _():
            passed_across(*PASSED[LAST])

        always = 4 * D_EXPERT + 2 * (D_EXPERT - MOST * STEP)
        sent(gate.at[0 : always // SHARDS, :], ici_send.at[0])
        times = 2 * MOST + sum(taken) - sum(left)
        for t in sorted({2 * MOST + sum(LEFT[lane][(k + 4) % Z] - LEFT[lane][k] for lane in range(2)) for k in range(Z)}):
            @pl.when(times == t)
            def _():
                sent(gate.at[0 : STEP * t // 2, 0 : 2 * WIDE], ici_send.at[1])
        sent(ring.at[c, y, x, 0:7], r_send.at[0])
        sent(held.at[0, 0:168, 0:768], r_send.at[1])

        def swapped(ref):
            sent(ref, core_sem.at[0])
            pltpu.make_async_remote_copy(ref, ref, core_sem.at[0], core_sem.at[1], device_id=near[MATE], device_id_type=MESH).wait_recv()

        @pl.when(odd)
        def _():
            sent(gate.at[0:TWICE, 0 : 2 * WIDE], ici_send.at[2])
            arrived(TWICE, passed_recv.at[LAST + 1])
            swapped(gate.at[0 : D_EXPERT - 2 * TWICE // SHARDS, :])

        @pl.when(even)
        def _():
            swapped(gate)


def store(gate, up, router, gate_out, up_out, router_out, sem):
    copies = [pltpu.make_async_copy(a, b, sem.at[i])
              for i, (a, b) in enumerate(((gate, gate_out), (up, up_out), (router, router_out)))]
    for copy in copies:
        copy.start()
    for copy in copies:
        copy.wait()


def local(w_gate, avg_gate, w_up, avg_up, mix_share, router_weight, router_gain):
    out = jax.ShapeDtypeStruct((D_EXPERT, D_MODEL), jnp.bfloat16)
    outs = (out, out, jax.ShapeDtypeStruct((EXPERTS, D_MODEL), jnp.bfloat16))
    hbm = pl.BlockSpec(memory_space=pltpu.HBM)
    vmem = pl.BlockSpec(memory_space=pltpu.VMEM)
    dma = pltpu.SemaphoreType.DMA
    gathered = pl.pallas_call(
        kernel,
        out_shape=outs,
        in_specs=[hbm] * 6 + [vmem],
        out_specs=(vmem,) * 3,
        scratch_shapes=[
            pltpu.VMEM((4, WIDE, D_EXPERT), jnp.float32),
            dma((len(GROUPS),)),
            pltpu.VMEM((2, 1, WIDE), jnp.float32),
            dma,
            pltpu.VMEM((2, Y, X, Z, 1, WIDE), jnp.float32),
            pltpu.VMEM((EXPERTS, D_MODEL), jnp.float32),
            pltpu.SemaphoreType.REGULAR((4,)),
            dma((len(GROUPS),)),
            dma((len(OTHER),)),
            dma((len(PASSED) + 2,)),
            dma((3,)),
            dma((2,)),
            dma((2,)),
            dma((9,)),
        ],
        compiler_params=pltpu.CompilerParams(
            collective_id=0, has_side_effects=True, vmem_limit_bytes=40 * 2**20),
        name="mix_and_gather",
    )(*(pltpu.with_memory_space_constraint(a, pltpu.HBM) for a in (
        w_gate, avg_gate, w_up, avg_up, router_weight.reshape(1, WIDE), router_gain.reshape(1, WIDE))),
      mix_share.reshape(1, 1))
    gate, up, router = pl.pallas_call(
        store,
        out_shape=outs,
        in_specs=[vmem] * 3,
        out_specs=(hbm,) * 3,
        scratch_shapes=[dma((3,))],
        compiler_params=pltpu.CompilerParams(vmem_limit_bytes=2**20),
        name="store",
    )(*gathered)
    return gate[None], up[None], router.T


def solution(mesh):
    return jax.shard_map(
        local,
        mesh=mesh,
        in_specs=(
            P("expert", "shard", None),
            P("expert", "shard", None),
            P("expert", "shard", None),
            P("expert", "shard", None),
            P("expert"),
            P("shard", "expert"),
            P("shard"),
        ),
        out_specs=(P("expert", None, None), P("expert", None, None), P()),
        check_vma=False,
    )
```

```python
import jax
import jax.numpy as jnp
from jax import lax
from jax.experimental import pallas as pl
from jax.experimental.pallas import tpu as pltpu
from jax.sharding import PartitionSpec as P

MESH = pl.DeviceIdType.MESH
D_MODEL, D_EXPERT, EXPERTS, SHARDS = 2048, 1024, 64, 8
WIDE = D_MODEL // SHARDS
ROWS = 128
CHUNKS = D_EXPERT // ROWS
X, Y, Z = 4, 8, 8
FORE, BACK, MATE, ZP, ZM, XP, XM, YP, YM, FORE_MATE, BACK_MATE = range(11)
OPPOSITE = (BACK, FORE, MATE, ZM, ZP, XM, XP, YM, YP, BACK_MATE, FORE_MATE)
TWICE = 64
GROUPS = ((0, 1), (1, 3), (4, 4))
OTHER = ((0, 2), (2, 6))
STEP, MOST = 64, 4
PASSED = ((MOST * STEP, 256), (512, 256), (768, 128), (896, 128 - TWICE), (1024 - TWICE, TWICE))
LAST = len(PASSED) - 1
LEFT = (0, 0, 0, 0, 0, 0, 4, 0), (3, 0, 0, 0, 2, 1, 0, 0)
LATE = 6


def kernel(wg, ag, wu, au, rw_any, gain_any, mix, gate, up, router, held, load_sem, small, small_sem, ring, flat,
           ready, first_recv, second_recv, passed_recv, ici_send, core_sem, r_send, r_recv):
    e, s = lax.axis_index("expert"), lax.axis_index("shard")
    x, y, z_lo = e & (X - 1), (e >> 2) & (Y - 1), e >> 5
    z_hi, c = s >> 1, s & 1
    z = 2 * z_hi + z_lo

    def columns_of(g):
        return pl.ds(GROUPS[g][0] * ROWS, GROUPS[g][1] * ROWS)

    for i, ref in enumerate((rw_any, gain_any)):
        pltpu.make_async_copy(ref, small.at[i], small_sem).start()
    for g in range(len(GROUPS)):
        for k in (1, 0):
            for i, ref in enumerate(((wg, ag), (wu, au))[k]):
                pltpu.make_async_copy(ref.at[0, :, columns_of(g)], held.at[2 * k + i, :, columns_of(g)], load_sem.at[g]).start()

    def loaded(g):
        ref = held.at[:, :, columns_of(g)]
        pltpu.make_async_copy(ref, ref, load_sem.at[g]).wait()

    def place(dx=0, dy=0, dz=0, dc=0):
        return (x + dx) & (X - 1), (y + dy) & (Y - 1), (z + dz) & (Z - 1), (c + dc) & 1

    def device(p):
        return {"expert": ((p[2] & 1) << 5) + (p[1] << 2) + p[0], "shard": (p[2] & 6) + p[3]}

    def rank(p):
        order = (p[2] << 7) + (p[1] << 4) + (p[0] << 2) + 2 - 2 * p[3]
        return jnp.where(order == 2, (LATE << 7) - 1, order)

    places = [place(dz=2), place(dz=-2), place(dc=1), place(dz=1), place(dz=-1), place(dx=1), place(dx=-1), place(dy=1), place(dy=-1),
              place(dz=2, dc=1), place(dz=-2, dc=1)]
    near = [device(p) for p in places]
    own_rank = rank(place())
    earlier = [rank(p) < own_rank for p in places]
    lanes = (FORE, BACK)

    barrier = pltpu.get_barrier_semaphore()
    for k in range(11):
        @pl.when(jnp.logical_not(earlier[k]))
        def _():
            pl.semaphore_signal(barrier, inc=1, device_id=near[k], device_id_type=MESH)
    def answer():
        before = sum(a.astype(jnp.int32) for a in earlier)

        @pl.when(before > 0)
        def _():
            pl.semaphore_wait(barrier, before)

        for k in range(11):
            @pl.when(earlier[k])
            def _():
                pl.semaphore_signal(ready.at[min(OPPOSITE[k], ZP)], inc=1, device_id=near[k], device_id_type=MESH)

    def allow(k):
        @pl.when(jnp.logical_not(earlier[k]))
        def _():
            pl.semaphore_wait(ready.at[k], 1)

    def allow_rest():
        after = sum(1 - earlier[k].astype(jnp.int32) for k in range(ZP, 11))

        @pl.when(after > 0)
        def _():
            pl.semaphore_wait(ready.at[ZP], after)

    share = mix[...]
    rest = 1.0 - share

    def columns(shard):
        return pl.ds(pl.multiple_of(shard * WIDE, WIDE), WIDE)

    def rows(j, n=1):
        return pl.ds(pl.multiple_of(j * ROWS, ROWS), n * ROWS)

    def compute(k, j):
        fresh = share * held[2 * k, :, rows(j)] + rest * held[2 * k + 1, :, rows(j)]
        (gate, up)[k][rows(j), columns(s)] = fresh.T.astype(jnp.bfloat16)

    def copy(k, shard, lo, n, to, send, recv):
        ref = (gate, up)[k].at[pl.ds(lo, n), columns(shard)]
        return pltpu.make_async_remote_copy(ref, ref, send, recv, device_id=near[to], device_id_type=MESH)

    def chunks(j, n):
        return j * ROWS, n * ROWS

    def first(lane, i):
        return copy(lane, s, *chunks(*GROUPS[i]), lanes[lane], ici_send.at[0], first_recv.at[i])

    def second(lane, i):
        return copy(1 - lane, s, *chunks(*OTHER[i]), lanes[lane], ici_send.at[0], second_recv.at[i])

    def passed(lane, p, shard):
        return copy(lane, shard, *PASSED[p], lanes[lane], ici_send.at[0], passed_recv.at[p])

    def shared(lane, i, shard, to):
        return copy(lane, shard, i * STEP, STEP, to, ici_send.at[1], passed_recv.at[LAST + 2])

    def across(k, shard, lo, n):
        return copy(k, shard, lo, n, MATE, core_sem.at[0], core_sem.at[1])

    def arrived(n, sem):
        ref = gate.at[0:n, 0 : 2 * WIDE]
        pltpu.make_async_remote_copy(ref, ref, core_sem.at[0], sem, device_id=near[MATE], device_id_type=MESH).wait_recv()

    def arriving(lane, far):
        return ((z_hi + (4 - far if lane == 0 else far)) & 3) * 2 + c

    def sent(ref, sem):
        pltpu.make_async_remote_copy(ref, ref, sem, core_sem.at[1], device_id=near[MATE], device_id_type=MESH).wait_send()

    def post(ref, to, i):
        return pltpu.make_async_remote_copy(
            ref, ref, r_send.at[min(i // 2, 1)], r_recv.at[i], device_id=near[to], device_id_type=MESH)

    def piece(k):
        return ring.at[c, y, x, (z + k) & (Z - 1)]

    def row(k):
        return ring.at[c, y, (x + k) & (X - 1)]

    def plane(k):
        return ring.at[c, (y + k) & (Y - 1)]

    def landed(ref, i):
        post(ref, MATE, i).wait_recv()

    even = (z & 1) == 0
    zeroth = jnp.logical_or(z < 2, z >= 6)

    def in_turn(order, do):
        for lane in range(2):
            @pl.when(zeroth if lane == order else jnp.logical_not(zeroth))
            def _():
                do(lane)

    def own_piece(lane):
        post(piece(0), lanes[lane], 0).start()

    def begin(order, *which):
        in_turn(order, lambda lane: [first(lane, i).start() for i in which])

    def begin_other(order, *which):
        in_turn(order, lambda lane: [second(lane, i).start() for i in which])

    both = jnp.logical_and(even, z >= 6)
    one = jnp.logical_and(even, z < 6)

    with jax.named_scope("first_chunk"):
        answer()
        loaded(0)
        compute(1, 0)
        compute(0, 0)
    with jax.named_scope("admit_first"):
        in_turn(0, lambda lane: allow(lanes[lane]))

        @pl.when(even)
        def _():
            begin(0, 0)

        @pl.when(both)
        def _():
            begin(1, 0)
    with jax.named_scope("compute"):
        def more(j, _):
            for k in (1, 0):
                compute(k, j)
            return 0

        def more_of(g):
            loaded(g)
            lax.fori_loop(GROUPS[g][0], sum(GROUPS[g]), more, 0)

        more_of(1)
        pltpu.make_async_copy(small, small, small_sem).wait()
        ring[c, y, x, z] = small[0] * small[1]
        in_turn(0, own_piece)

        @pl.when(even)
        def _():
            begin(0, 1)

        @pl.when(both)
        def _():
            in_turn(1, own_piece)
            begin(1, 1)

        @pl.when(even)
        def _():
            begin_other(0, 0)

        more_of(2)
    with jax.named_scope("admit_second"):
        in_turn(1, lambda lane: allow(lanes[lane]))

        @pl.when(jnp.logical_not(both))
        def _():
            in_turn(1, own_piece)

        @pl.when(one)
        def _():
            begin(1, 0, 1)

        @pl.when(even)
        def _():
            begin_other(1, 0)
    with jax.named_scope("z_steps"):
        allow_rest()
        post(piece(0), ZP, 1).start()
        post(piece(0), ZM, 1).start()
        landed(ring.at[c, y, x, 0:2], 0)
        post(piece(-2), ZP, 1).start()
        post(piece(2), ZM, 1).start()
        post(piece(-2), FORE, 1).start()
    with jax.named_scope("own"):
        @pl.when(jnp.logical_not(even))
        def _():
            for order in range(2):
                begin(order, 0, 1)
                begin_other(order, 0)

        for order in range(2):
            begin(order, 2)
            begin_other(order, 1)
    with jax.named_scope("mate_own"):
        allow(MATE)
        for k in range(2):
            across(k, s, 0, D_EXPERT).start()

    def at_plane(table):
        return sum(jnp.where(z == k, v, 0) for k, v in enumerate(table) if v) + jnp.where(z < 0, 1, 0)

    left = [at_plane(LEFT[lane]) for lane in range(2)]
    taken = [at_plane([LEFT[lane][(k + 4) % Z] for k in range(Z)]) for lane in range(2)]

    odd = jnp.logical_not(even)

    def own_arrived(i):
        with jax.named_scope(f"half_a{i}"):
            start, length = chunks(*GROUPS[i])
            arrived(length, first_recv.at[i])
            for lane in range(2):
                shard = arriving(lane, 1)
                for j in range(MOST):
                    if start <= j * STEP < start + length:
                        @pl.when(j >= left[lane])
                        def _():
                            shared(lane, j, shard, lanes[lane]).start()
                for p, (lo, n) in enumerate(PASSED):
                    if start <= lo < start + length:
                        passed(lane, p, shard).start()
                        if p == LAST:
                            @pl.when(odd)
                            def _():
                                copy(lane, shard, lo, n, (FORE_MATE, BACK_MATE)[lane], ici_send.at[2], passed_recv.at[LAST + 1]).start()
                across(lane, shard, start, length).start()

    def other_arrived(i):
        with jax.named_scope(f"half_b{i}"):
            start, length = chunks(*OTHER[i])
            arrived(length, second_recv.at[i])
            for lane in range(2):
                for j in range(MOST):
                    if start <= j * STEP < start + length and max(LEFT[lane]) > j:
                        @pl.when(j < taken[lane])
                        def _():
                            shared(lane, j, arriving(1 - lane, 1), lanes[1 - lane]).start()
            for lane in range(2):
                across(1 - lane, arriving(lane, 1), start, length).start()

    def router_rest():
        with jax.named_scope("router_x1"):
            landed(ring.at[c, y, x, 0:5], 1)
            post(row(0), XP, 2).start()
            post(row(0), XM, 2).start()
        with jax.named_scope("router_x2"):
            landed(ring.at[c, y, 0:2], 2)
            post(row(-1), XP, 3).start()
        with jax.named_scope("router_y1"):
            landed(ring.at[c, y, 0], 3)
            post(plane(0), YP, 4).start()
            post(plane(0), YM, 4).start()
        for i in range(3):
            with jax.named_scope(f"router_y{i + 2}"):
                landed(ring.at[c, 0:2], 4 + i)
                post(plane(-1 - i), YP, 5 + i).start()
                if i < 2:
                    post(plane(1 + i), YM, 5 + i).start()
        with jax.named_scope("router_mate"):
            landed(ring.at[c, 0], 7)
            post(ring.at[c], MATE, 8).start()

    def arrivals():
        own_arrived(0)
        own_arrived(1)
        other_arrived(0)
        own_arrived(2)

    @pl.when(even)
    def _():
        arrivals()
        router_rest()
        other_arrived(1)

    @pl.when(jnp.logical_not(even))
    def _():
        router_rest()
        arrivals()
        other_arrived(1)

    with jax.named_scope("router_end"):
        landed(ring.at[1 - c], 8)

        def lay(i, _):
            yy, xx = i >> 2, i & (X - 1)
            for zz in range(Z):
                for cc in range(2):
                    lo = (2 * (zz // 2) + cc) * WIDE
                    flat[pl.ds((zz % 2) * (Y * X) + i, 1), lo : lo + WIDE] = ring[cc, yy, xx, zz]
            return 0

        lax.fori_loop(0, Y * X, lay, 0)
        router[...] = flat[...].astype(jnp.bfloat16)
    def passed_across(lo, n):
        for lane in range(2):
            across(lane, arriving(lane, 2), lo, n).start()

    with jax.named_scope("shared"):
        arrived(MOST * STEP, passed_recv.at[LAST + 2])
        passed_across(0, MOST * STEP)
    for p, (lo, n) in enumerate(PASSED):
        with jax.named_scope(f"passed{p}"):
            arrived(n, passed_recv.at[p])
            if p < LAST:
                passed_across(lo, n)

    with jax.named_scope("finish"):
        @pl.when(even)
        def _():
            passed_across(*PASSED[LAST])

        always = 4 * D_EXPERT + 2 * (D_EXPERT - MOST * STEP)
        sent(gate.at[0 : always // SHARDS, :], ici_send.at[0])
        times = 2 * MOST + sum(taken) - sum(left)
        for t in sorted({2 * MOST + sum(LEFT[lane][(k + 4) % Z] - LEFT[lane][k] for lane in range(2)) for k in range(Z)}):
            @pl.when(times == t)
            def _():
                sent(gate.at[0 : STEP * t // 2, 0 : 2 * WIDE], ici_send.at[1])
        sent(ring.at[c, y, x, 0:7], r_send.at[0])
        sent(held.at[0, 0:168, 0:768], r_send.at[1])

        def swapped(ref):
            sent(ref, core_sem.at[0])
            pltpu.make_async_remote_copy(ref, ref, core_sem.at[0], core_sem.at[1], device_id=near[MATE], device_id_type=MESH).wait_recv()

        @pl.when(odd)
        def _():
            sent(gate.at[0:TWICE, 0 : 2 * WIDE], ici_send.at[2])
            arrived(TWICE, passed_recv.at[LAST + 1])
            swapped(gate.at[0 : D_EXPERT - 2 * TWICE // SHARDS, :])

        @pl.when(even)
        def _():
            swapped(gate)


def store(gate, up, router, gate_out, up_out, router_out, sem):
    copies = [pltpu.make_async_copy(a, b, sem.at[i])
              for i, (a, b) in enumerate(((gate, gate_out), (up, up_out), (router, router_out)))]
    for copy in copies:
        copy.start()
    for copy in copies:
        copy.wait()


def local(w_gate, avg_gate, w_up, avg_up, mix_share, router_weight, router_gain):
    out = jax.ShapeDtypeStruct((D_EXPERT, D_MODEL), jnp.bfloat16)
    outs = (out, out, jax.ShapeDtypeStruct((EXPERTS, D_MODEL), jnp.bfloat16))
    hbm = pl.BlockSpec(memory_space=pltpu.HBM)
    vmem = pl.BlockSpec(memory_space=pltpu.VMEM)
    dma = pltpu.SemaphoreType.DMA
    gathered = pl.pallas_call(
        kernel,
        out_shape=outs,
        in_specs=[hbm] * 6 + [vmem],
        out_specs=(vmem,) * 3,
        scratch_shapes=[
            pltpu.VMEM((4, WIDE, D_EXPERT), jnp.float32),
            dma((len(GROUPS),)),
            pltpu.VMEM((2, 1, WIDE), jnp.float32),
            dma,
            pltpu.VMEM((2, Y, X, Z, 1, WIDE), jnp.float32),
            pltpu.VMEM((EXPERTS, D_MODEL), jnp.float32),
            pltpu.SemaphoreType.REGULAR((4,)),
            dma((len(GROUPS),)),
            dma((len(OTHER),)),
            dma((len(PASSED) + 2,)),
            dma((3,)),
            dma((2,)),
            dma((2,)),
            dma((9,)),
        ],
        compiler_params=pltpu.CompilerParams(
            collective_id=0, has_side_effects=True, vmem_limit_bytes=40 * 2**20),
        name="mix_and_gather",
    )(*(pltpu.with_memory_space_constraint(a, pltpu.HBM) for a in (
        w_gate, avg_gate, w_up, avg_up, router_weight.reshape(1, WIDE), router_gain.reshape(1, WIDE))),
      mix_share.reshape(1, 1))
    gate, up, router = pl.pallas_call(
        store,
        out_shape=outs,
        in_specs=[vmem] * 3,
        out_specs=(hbm,) * 3,
        scratch_shapes=[dma((3,))],
        compiler_params=pltpu.CompilerParams(vmem_limit_bytes=2**20),
        name="store",
    )(*gathered)
    return gate[None], up[None], router.T


def solution(mesh):
    return jax.shard_map(
        local,
        mesh=mesh,
        in_specs=(
            P("expert", "shard", None),
            P("expert", "shard", None),
            P("expert", "shard", None),
            P("expert", "shard", None),
            P("expert"),
            P("shard", "expert"),
            P("shard"),
        ),
        out_specs=(P("expert", None, None), P("expert", None, None), P()),
        check_vma=False,
    )
```

```python
import jax
import jax.numpy as jnp
from jax import lax
from jax.experimental import pallas as pl
from jax.experimental.pallas import tpu as pltpu
from jax.sharding import PartitionSpec as P

MESH = pl.DeviceIdType.MESH
D_MODEL, D_EXPERT, EXPERTS, SHARDS = 2048, 1024, 64, 8
WIDE = D_MODEL // SHARDS
ROWS = 128
CHUNKS = D_EXPERT // ROWS
X, Y, Z = 4, 8, 8
FORE, BACK, MATE, ZP, ZM, XP, XM, YP, YM, FORE_MATE, BACK_MATE = range(11)
OPPOSITE = (BACK, FORE, MATE, ZM, ZP, XM, XP, YM, YP, BACK_MATE, FORE_MATE)
TWICE = 64
GROUPS = ((0, 1), (1, 3), (4, 4))
OTHER = ((0, 2), (2, 6))
STEP, MOST = 64, 4
PASSED = ((MOST * STEP, 256), (512, 256), (768, 256 - TWICE), (1024 - TWICE, TWICE))
LAST = len(PASSED) - 1
LEFT = (0, 0, 0, 0, 0, 0, 4, 0), (3, 0, 0, 0, 2, 1, 0, 0)
LATE = 6


def kernel(wg, ag, wu, au, rw_any, gain_any, mix, gate, up, router, held, load_sem, small, small_sem, ring, flat,
           ready, first_recv, second_recv, passed_recv, ici_send, core_sem, r_send, r_recv):
    e, s = lax.axis_index("expert"), lax.axis_index("shard")
    x, y, z_lo = e & (X - 1), (e >> 2) & (Y - 1), e >> 5
    z_hi, c = s >> 1, s & 1
    z = 2 * z_hi + z_lo

    def columns_of(g):
        return pl.ds(GROUPS[g][0] * ROWS, GROUPS[g][1] * ROWS)

    for i, ref in enumerate((rw_any, gain_any)):
        pltpu.make_async_copy(ref, small.at[i], small_sem).start()
    for g in range(len(GROUPS)):
        for k in (1, 0):
            for i, ref in enumerate(((wg, ag), (wu, au))[k]):
                pltpu.make_async_copy(ref.at[0, :, columns_of(g)], held.at[2 * k + i, :, columns_of(g)], load_sem.at[g]).start()

    def loaded(g):
        ref = held.at[:, :, columns_of(g)]
        pltpu.make_async_copy(ref, ref, load_sem.at[g]).wait()

    def place(dx=0, dy=0, dz=0, dc=0):
        return (x + dx) & (X - 1), (y + dy) & (Y - 1), (z + dz) & (Z - 1), (c + dc) & 1

    def device(p):
        return {"expert": ((p[2] & 1) << 5) + (p[1] << 2) + p[0], "shard": (p[2] & 6) + p[3]}

    def rank(p):
        order = (p[2] << 7) + (p[1] << 4) + (p[0] << 2) + 2 - 2 * p[3]
        return jnp.where(order == 2, (LATE << 7) - 1, order)

    places = [place(dz=2), place(dz=-2), place(dc=1), place(dz=1), place(dz=-1), place(dx=1), place(dx=-1), place(dy=1), place(dy=-1),
              place(dz=2, dc=1), place(dz=-2, dc=1)]
    near = [device(p) for p in places]
    own_rank = rank(place())
    earlier = [rank(p) < own_rank for p in places]
    lanes = (FORE, BACK)

    barrier = pltpu.get_barrier_semaphore()
    for k in range(11):
        @pl.when(jnp.logical_not(earlier[k]))
        def _():
            pl.semaphore_signal(barrier, inc=1, device_id=near[k], device_id_type=MESH)
    def answer():
        before = sum(a.astype(jnp.int32) for a in earlier)

        @pl.when(before > 0)
        def _():
            pl.semaphore_wait(barrier, before)

        for k in range(11):
            @pl.when(earlier[k])
            def _():
                pl.semaphore_signal(ready.at[min(OPPOSITE[k], ZP)], inc=1, device_id=near[k], device_id_type=MESH)

    def allow(k):
        @pl.when(jnp.logical_not(earlier[k]))
        def _():
            pl.semaphore_wait(ready.at[k], 1)

    def allow_rest():
        after = sum(1 - earlier[k].astype(jnp.int32) for k in range(ZP, 11))

        @pl.when(after > 0)
        def _():
            pl.semaphore_wait(ready.at[ZP], after)

    share = mix[...]
    rest = 1.0 - share

    def columns(shard):
        return pl.ds(pl.multiple_of(shard * WIDE, WIDE), WIDE)

    def rows(j, n=1):
        return pl.ds(pl.multiple_of(j * ROWS, ROWS), n * ROWS)

    def compute(k, j):
        fresh = share * held[2 * k, :, rows(j)] + rest * held[2 * k + 1, :, rows(j)]
        (gate, up)[k][rows(j), columns(s)] = fresh.T.astype(jnp.bfloat16)

    def copy(k, shard, lo, n, to, send, recv):
        ref = (gate, up)[k].at[pl.ds(lo, n), columns(shard)]
        return pltpu.make_async_remote_copy(ref, ref, send, recv, device_id=near[to], device_id_type=MESH)

    def chunks(j, n):
        return j * ROWS, n * ROWS

    def first(lane, i):
        return copy(lane, s, *chunks(*GROUPS[i]), lanes[lane], ici_send, first_recv.at[i])

    def second(lane, i):
        return copy(1 - lane, s, *chunks(*OTHER[i]), lanes[lane], ici_send, second_recv.at[i])

    def passed(lane, p, shard):
        return copy(lane, shard, *PASSED[p], lanes[lane], ici_send, passed_recv.at[p])

    def shared(lane, i, shard, to):
        return copy(lane, shard, i * STEP, STEP, to, ici_send, passed_recv.at[LAST + 2])

    def across(k, shard, lo, n):
        return copy(k, shard, lo, n, MATE, core_sem.at[0], core_sem.at[1])

    def arrived(n, sem):
        ref = gate.at[0:n, 0 : 2 * WIDE]
        pltpu.make_async_remote_copy(ref, ref, core_sem.at[0], sem, device_id=near[MATE], device_id_type=MESH).wait_recv()

    def arriving(lane, far):
        return ((z_hi + (4 - far if lane == 0 else far)) & 3) * 2 + c

    def sent(ref, sem):
        pltpu.make_async_remote_copy(ref, ref, sem, core_sem.at[1], device_id=near[MATE], device_id_type=MESH).wait_send()

    def post(ref, to, i):
        return pltpu.make_async_remote_copy(
            ref, ref, r_send.at[min(i // 2, 1)], r_recv.at[i], device_id=near[to], device_id_type=MESH)

    def piece(k):
        return ring.at[c, y, x, (z + k) & (Z - 1)]

    def row(k):
        return ring.at[c, y, (x + k) & (X - 1)]

    def plane(k):
        return ring.at[c, (y + k) & (Y - 1)]

    def landed(ref, i):
        post(ref, MATE, i).wait_recv()

    even = (z & 1) == 0
    zeroth = jnp.logical_or(z < 2, z >= 6)

    def in_turn(order, do):
        for lane in range(2):
            @pl.when(zeroth if lane == order else jnp.logical_not(zeroth))
            def _():
                do(lane)

    def own_piece(lane):
        post(piece(0), lanes[lane], 0).start()

    def begin(order, *which):
        in_turn(order, lambda lane: [first(lane, i).start() for i in which])

    def begin_other(order, *which):
        in_turn(order, lambda lane: [second(lane, i).start() for i in which])

    both = jnp.logical_and(even, z >= 6)
    one = jnp.logical_and(even, z < 6)

    with jax.named_scope("first_chunk"):
        answer()
        loaded(0)
        compute(1, 0)
        compute(0, 0)
    with jax.named_scope("admit_first"):
        in_turn(0, lambda lane: allow(lanes[lane]))

        @pl.when(even)
        def _():
            begin(0, 0)

        @pl.when(both)
        def _():
            begin(1, 0)
    with jax.named_scope("compute"):
        def more(j, _):
            for k in (1, 0):
                compute(k, j)
            return 0

        def more_of(g):
            loaded(g)
            lax.fori_loop(GROUPS[g][0], sum(GROUPS[g]), more, 0)

        more_of(1)
        pltpu.make_async_copy(small, small, small_sem).wait()
        ring[c, y, x, z] = small[0] * small[1]
        in_turn(0, own_piece)

        @pl.when(even)
        def _():
            begin(0, 1)

        @pl.when(both)
        def _():
            in_turn(1, own_piece)
            begin(1, 1)

        @pl.when(even)
        def _():
            begin_other(0, 0)

        more_of(2)
    with jax.named_scope("admit_second"):
        in_turn(1, lambda lane: allow(lanes[lane]))

        @pl.when(jnp.logical_not(both))
        def _():
            in_turn(1, own_piece)

        @pl.when(one)
        def _():
            begin(1, 0, 1)

        @pl.when(even)
        def _():
            begin_other(1, 0)
    with jax.named_scope("z_steps"):
        allow_rest()
        post(piece(0), ZP, 1).start()
        post(piece(0), ZM, 1).start()
        landed(ring.at[c, y, x, 0:2], 0)
        post(piece(-2), ZP, 1).start()
        post(piece(2), ZM, 1).start()
        post(piece(-2), FORE, 1).start()
    with jax.named_scope("own"):
        @pl.when(jnp.logical_not(even))
        def _():
            for order in range(2):
                begin(order, 0, 1)
                begin_other(order, 0)

        for order in range(2):
            begin(order, 2)
            begin_other(order, 1)
    with jax.named_scope("mate_own"):
        allow(MATE)
        for k in range(2):
            across(k, s, 0, D_EXPERT).start()

    def at_plane(table):
        return sum(jnp.where(z == k, v, 0) for k, v in enumerate(table) if v) + jnp.where(z < 0, 1, 0)

    left = [at_plane(LEFT[lane]) for lane in range(2)]
    taken = [at_plane([LEFT[lane][(k + 4) % Z] for k in range(Z)]) for lane in range(2)]

    odd = jnp.logical_not(even)

    def own_arrived(i):
        with jax.named_scope(f"half_a{i}"):
            start, length = chunks(*GROUPS[i])
            arrived(length, first_recv.at[i])
            for lane in range(2):
                shard = arriving(lane, 1)
                for j in range(MOST):
                    if start <= j * STEP < start + length:
                        @pl.when(j >= left[lane])
                        def _():
                            shared(lane, j, shard, lanes[lane]).start()
                for p, (lo, n) in enumerate(PASSED):
                    if start <= lo < start + length:
                        passed(lane, p, shard).start()
                        if p == LAST:
                            @pl.when(z == (7, 3)[lane])
                            def _():
                                copy(lane, shard, lo, n, (FORE_MATE, BACK_MATE)[lane], ici_send, passed_recv.at[LAST + 1]).start()
                across(lane, shard, start, length).start()

    def other_arrived(i):
        with jax.named_scope(f"half_b{i}"):
            start, length = chunks(*OTHER[i])
            arrived(length, second_recv.at[i])
            for lane in range(2):
                for j in range(MOST):
                    if start <= j * STEP < start + length and max(LEFT[lane]) > j:
                        @pl.when(j < taken[lane])
                        def _():
                            shared(lane, j, arriving(1 - lane, 1), lanes[1 - lane]).start()
            for lane in range(2):
                across(1 - lane, arriving(lane, 1), start, length).start()

    def router_rest():
        with jax.named_scope("router_x1"):
            landed(ring.at[c, y, x, 0:5], 1)
            post(row(0), XP, 2).start()
            post(row(0), XM, 2).start()
        with jax.named_scope("router_x2"):
            landed(ring.at[c, y, 0:2], 2)
            post(row(-1), XP, 3).start()
        with jax.named_scope("router_y1"):
            landed(ring.at[c, y, 0], 3)
            post(plane(0), YP, 4).start()
            post(plane(0), YM, 4).start()
        for i in range(3):
            with jax.named_scope(f"router_y{i + 2}"):
                landed(ring.at[c, 0:2], 4 + i)
                post(plane(-1 - i), YP, 5 + i).start()
                if i < 2:
                    post(plane(1 + i), YM, 5 + i).start()
        with jax.named_scope("router_mate"):
            landed(ring.at[c, 0], 7)
            post(ring.at[c], MATE, 8).start()

    def arrivals():
        own_arrived(0)
        own_arrived(1)
        other_arrived(0)
        own_arrived(2)

    @pl.when(even)
    def _():
        arrivals()
        router_rest()
        other_arrived(1)

    @pl.when(jnp.logical_not(even))
    def _():
        router_rest()
        arrivals()
        other_arrived(1)

    with jax.named_scope("router_end"):
        landed(ring.at[1 - c], 8)

        def lay(i, _):
            yy, xx = i >> 2, i & (X - 1)
            for zz in range(Z):
                for cc in range(2):
                    lo = (2 * (zz // 2) + cc) * WIDE
                    flat[pl.ds((zz % 2) * (Y * X) + i, 1), lo : lo + WIDE] = ring[cc, yy, xx, zz]
            return 0

        lax.fori_loop(0, Y * X, lay, 0)
        router[...] = flat[...].astype(jnp.bfloat16)
    def passed_across(lo, n):
        for lane in range(2):
            across(lane, arriving(lane, 2), lo, n).start()

    with jax.named_scope("shared"):
        arrived(MOST * STEP, passed_recv.at[LAST + 2])
        passed_across(0, MOST * STEP)
    for p, (lo, n) in enumerate(PASSED):
        with jax.named_scope(f"passed{p}"):
            arrived(n, passed_recv.at[p])
            if p < LAST:
                passed_across(lo, n)

    with jax.named_scope("finish"):
        twice = z == 1

        @pl.when(jnp.logical_not(twice))
        def _():
            passed_across(*PASSED[LAST])

        def rows_sent(k):
            shared_rows = STEP * (2 * MOST + sum(LEFT[lane][(k + 4) % Z] - LEFT[lane][k] for lane in range(2)))
            return 4 * D_EXPERT + 2 * (D_EXPERT - MOST * STEP) + shared_rows + TWICE * (k in (3, 7))

        for n in sorted({rows_sent(k) for k in range(Z)}):
            @pl.when(at_plane([int(rows_sent(k) == n) for k in range(Z)]) > 0)
            def _():
                sent(gate.at[0 : n // SHARDS, :], ici_send)
        sent(ring.at[c, y, x, 0:7], r_send.at[0])
        sent(held.at[0, 0:168, 0:768], r_send.at[1])

        def swapped(ref):
            sent(ref, core_sem.at[0])
            pltpu.make_async_remote_copy(ref, ref, core_sem.at[0], core_sem.at[1], device_id=near[MATE], device_id_type=MESH).wait_recv()

        @pl.when(twice)
        def _():
            arrived(TWICE, passed_recv.at[LAST + 1])
            swapped(gate.at[0 : D_EXPERT - 2 * TWICE // SHARDS, :])

        @pl.when(jnp.logical_not(twice))
        def _():
            swapped(gate)


def store(gate, up, router, gate_out, up_out, router_out, sem):
    copies = [pltpu.make_async_copy(a, b, sem.at[i])
              for i, (a, b) in enumerate(((gate, gate_out), (up, up_out), (router, router_out)))]
    for copy in copies:
        copy.start()
    for copy in copies:
        copy.wait()


def local(w_gate, avg_gate, w_up, avg_up, mix_share, router_weight, router_gain):
    out = jax.ShapeDtypeStruct((D_EXPERT, D_MODEL), jnp.bfloat16)
    outs = (out, out, jax.ShapeDtypeStruct((EXPERTS, D_MODEL), jnp.bfloat16))
    hbm = pl.BlockSpec(memory_space=pltpu.HBM)
    vmem = pl.BlockSpec(memory_space=pltpu.VMEM)
    dma = pltpu.SemaphoreType.DMA
    gathered = pl.pallas_call(
        kernel,
        out_shape=outs,
        in_specs=[hbm] * 6 + [vmem],
        out_specs=(vmem,) * 3,
        scratch_shapes=[
            pltpu.VMEM((4, WIDE, D_EXPERT), jnp.float32),
            dma((len(GROUPS),)),
            pltpu.VMEM((2, 1, WIDE), jnp.float32),
            dma,
            pltpu.VMEM((2, Y, X, Z, 1, WIDE), jnp.float32),
            pltpu.VMEM((EXPERTS, D_MODEL), jnp.float32),
            pltpu.SemaphoreType.REGULAR((4,)),
            dma((len(GROUPS),)),
            dma((len(OTHER),)),
            dma((len(PASSED) + 2,)),
            dma,
            dma((2,)),
            dma((2,)),
            dma((9,)),
        ],
        compiler_params=pltpu.CompilerParams(
            collective_id=0, has_side_effects=True, vmem_limit_bytes=40 * 2**20),
        name="mix_and_gather",
    )(*(pltpu.with_memory_space_constraint(a, pltpu.HBM) for a in (
        w_gate, avg_gate, w_up, avg_up, router_weight.reshape(1, WIDE), router_gain.reshape(1, WIDE))),
      mix_share.reshape(1, 1))
    gate, up, router = pl.pallas_call(
        store,
        out_shape=outs,
        in_specs=[vmem] * 3,
        out_specs=(hbm,) * 3,
        scratch_shapes=[dma((3,))],
        compiler_params=pltpu.CompilerParams(vmem_limit_bytes=2**20),
        name="store",
    )(*gathered)
    return gate[None], up[None], router.T


def solution(mesh):
    return jax.shard_map(
        local,
        mesh=mesh,
        in_specs=(
            P("expert", "shard", None),
            P("expert", "shard", None),
            P("expert", "shard", None),
            P("expert", "shard", None),
            P("expert"),
            P("shard", "expert"),
            P("shard"),
        ),
        out_specs=(P("expert", None, None), P("expert", None, None), P()),
        check_vma=False,
    )
```

```python
import jax
import jax.numpy as jnp
from jax import lax
from jax.experimental import pallas as pl
from jax.experimental.pallas import tpu as pltpu
from jax.sharding import PartitionSpec as P

MESH = pl.DeviceIdType.MESH
D_MODEL, D_EXPERT, EXPERTS, SHARDS = 2048, 1024, 64, 8
WIDE = D_MODEL // SHARDS
ROWS = 128
CHUNKS = D_EXPERT // ROWS
X, Y, Z = 4, 8, 8
FORE, BACK, MATE, ZP, ZM, XP, XM, YP, YM, FORE_MATE, BACK_MATE = range(11)
OPPOSITE = (BACK, FORE, MATE, ZM, ZP, XM, XP, YM, YP, BACK_MATE, FORE_MATE)
TWICE = 64
GROUPS = ((0, 1), (1, 3), (4, 4))
OTHER = ((0, 2), (2, 6))
STEP, MOST = 64, 4
PASSED = ((MOST * STEP, 256), (512, 256), (768, 128), (896, 128 - TWICE), (1024 - TWICE, TWICE))
LAST = len(PASSED) - 1
LEFT = (0, 0, 0, 0, 0, 0, 4, 0), (3, 0, 0, 0, 2, 1, 0, 0)
LATE = 6


def kernel(wg, ag, wu, au, rw_any, gain_any, mix, gate, up, router, held, load_sem, small, small_sem, ring, flat,
           ready, first_recv, second_recv, passed_recv, ici_send, core_sem, r_send, r_recv):
    e, s = lax.axis_index("expert"), lax.axis_index("shard")
    x, y, z_lo = e & (X - 1), (e >> 2) & (Y - 1), e >> 5
    z_hi, c = s >> 1, s & 1
    z = 2 * z_hi + z_lo

    def columns_of(g):
        return pl.ds(GROUPS[g][0] * ROWS, GROUPS[g][1] * ROWS)

    for i, ref in enumerate((rw_any, gain_any)):
        pltpu.make_async_copy(ref, small.at[i], small_sem).start()
    for g in range(len(GROUPS)):
        for k in (1, 0):
            for i, ref in enumerate(((wg, ag), (wu, au))[k]):
                pltpu.make_async_copy(ref.at[0, :, columns_of(g)], held.at[2 * k + i, :, columns_of(g)], load_sem.at[g]).start()

    def loaded(g):
        ref = held.at[:, :, columns_of(g)]
        pltpu.make_async_copy(ref, ref, load_sem.at[g]).wait()

    def place(dx=0, dy=0, dz=0, dc=0):
        return (x + dx) & (X - 1), (y + dy) & (Y - 1), (z + dz) & (Z - 1), (c + dc) & 1

    def device(p):
        return {"expert": ((p[2] & 1) << 5) + (p[1] << 2) + p[0], "shard": (p[2] & 6) + p[3]}

    def rank(p):
        order = (p[2] << 7) + (p[1] << 4) + (p[0] << 2) + 2 - 2 * p[3]
        return jnp.where(order == 2, (LATE << 7) - 1, order)

    places = [place(dz=2), place(dz=-2), place(dc=1), place(dz=1), place(dz=-1), place(dx=1), place(dx=-1), place(dy=1), place(dy=-1),
              place(dz=2, dc=1), place(dz=-2, dc=1)]
    near = [device(p) for p in places]
    own_rank = rank(place())
    earlier = [rank(p) < own_rank for p in places]
    lanes = (FORE, BACK)

    barrier = pltpu.get_barrier_semaphore()
    for k in range(11):
        @pl.when(jnp.logical_not(earlier[k]))
        def _():
            pl.semaphore_signal(barrier, inc=1, device_id=near[k], device_id_type=MESH)
    def answer():
        before = sum(a.astype(jnp.int32) for a in earlier)

        @pl.when(before > 0)
        def _():
            pl.semaphore_wait(barrier, before)

        for k in range(11):
            @pl.when(earlier[k])
            def _():
                pl.semaphore_signal(ready.at[min(OPPOSITE[k], ZP)], inc=1, device_id=near[k], device_id_type=MESH)

    def allow(k):
        @pl.when(jnp.logical_not(earlier[k]))
        def _():
            pl.semaphore_wait(ready.at[k], 1)

    def allow_rest():
        after = sum(1 - earlier[k].astype(jnp.int32) for k in range(ZP, 11))

        @pl.when(after > 0)
        def _():
            pl.semaphore_wait(ready.at[ZP], after)

    share = mix[...]
    rest = 1.0 - share

    def columns(shard):
        return pl.ds(pl.multiple_of(shard * WIDE, WIDE), WIDE)

    def rows(j, n=1):
        return pl.ds(pl.multiple_of(j * ROWS, ROWS), n * ROWS)

    def compute(k, j):
        fresh = share * held[2 * k, :, rows(j)] + rest * held[2 * k + 1, :, rows(j)]
        (gate, up)[k][rows(j), columns(s)] = fresh.T.astype(jnp.bfloat16)

    def copy(k, shard, lo, n, to, send, recv):
        ref = (gate, up)[k].at[pl.ds(lo, n), columns(shard)]
        return pltpu.make_async_remote_copy(ref, ref, send, recv, device_id=near[to], device_id_type=MESH)

    def chunks(j, n):
        return j * ROWS, n * ROWS

    def first(lane, i):
        return copy(lane, s, *chunks(*GROUPS[i]), lanes[lane], ici_send, first_recv.at[i])

    def second(lane, i):
        return copy(1 - lane, s, *chunks(*OTHER[i]), lanes[lane], ici_send, second_recv.at[i])

    def passed(lane, p, shard):
        return copy(lane, shard, *PASSED[p], lanes[lane], ici_send, passed_recv.at[p])

    def shared(lane, i, shard, to):
        return copy(lane, shard, i * STEP, STEP, to, ici_send, passed_recv.at[LAST + 2])

    def across(k, shard, lo, n):
        return copy(k, shard, lo, n, MATE, core_sem.at[0], core_sem.at[1])

    def arrived(n, sem):
        ref = gate.at[0:n, 0 : 2 * WIDE]
        pltpu.make_async_remote_copy(ref, ref, core_sem.at[0], sem, device_id=near[MATE], device_id_type=MESH).wait_recv()

    def arriving(lane, far):
        return ((z_hi + (4 - far if lane == 0 else far)) & 3) * 2 + c

    def sent(ref, sem):
        pltpu.make_async_remote_copy(ref, ref, sem, core_sem.at[1], device_id=near[MATE], device_id_type=MESH).wait_send()

    def post(ref, to, i):
        return pltpu.make_async_remote_copy(
            ref, ref, r_send.at[min(i // 2, 1)], r_recv.at[i], device_id=near[to], device_id_type=MESH)

    def piece(k):
        return ring.at[c, y, x, (z + k) & (Z - 1)]

    def row(k):
        return ring.at[c, y, (x + k) & (X - 1)]

    def plane(k):
        return ring.at[c, (y + k) & (Y - 1)]

    def landed(ref, i):
        post(ref, MATE, i).wait_recv()

    even = (z & 1) == 0
    zeroth = jnp.logical_or(z < 2, z >= 6)

    def in_turn(order, do):
        for lane in range(2):
            @pl.when(zeroth if lane == order else jnp.logical_not(zeroth))
            def _():
                do(lane)

    def own_piece(lane):
        post(piece(0), lanes[lane], 0).start()

    def begin(order, *which):
        in_turn(order, lambda lane: [first(lane, i).start() for i in which])

    def begin_other(order, *which):
        in_turn(order, lambda lane: [second(lane, i).start() for i in which])

    both = jnp.logical_and(even, z >= 6)
    one = jnp.logical_and(even, z < 6)

    with jax.named_scope("first_chunk"):
        answer()
        loaded(0)
        compute(1, 0)
        compute(0, 0)
    with jax.named_scope("admit_first"):
        in_turn(0, lambda lane: allow(lanes[lane]))

        @pl.when(even)
        def _():
            begin(0, 0)

        @pl.when(both)
        def _():
            begin(1, 0)
    with jax.named_scope("compute"):
        def more(j, _):
            for k in (1, 0):
                compute(k, j)
            return 0

        def more_of(g):
            loaded(g)
            lax.fori_loop(GROUPS[g][0], sum(GROUPS[g]), more, 0)

        more_of(1)
        pltpu.make_async_copy(small, small, small_sem).wait()
        ring[c, y, x, z] = small[0] * small[1]
        in_turn(0, own_piece)

        @pl.when(even)
        def _():
            begin(0, 1)

        @pl.when(both)
        def _():
            in_turn(1, own_piece)
            begin(1, 1)

        @pl.when(even)
        def _():
            begin_other(0, 0)

        more_of(2)
    with jax.named_scope("admit_second"):
        in_turn(1, lambda lane: allow(lanes[lane]))

        @pl.when(jnp.logical_not(both))
        def _():
            in_turn(1, own_piece)

        @pl.when(one)
        def _():
            begin(1, 0, 1)

        @pl.when(even)
        def _():
            begin_other(1, 0)
    with jax.named_scope("z_steps"):
        allow_rest()
        post(piece(0), ZP, 1).start()
        post(piece(0), ZM, 1).start()
        landed(ring.at[c, y, x, 0:2], 0)
        post(piece(-2), ZP, 1).start()
        post(piece(2), ZM, 1).start()
        post(piece(-2), FORE, 1).start()
    with jax.named_scope("own"):
        @pl.when(jnp.logical_not(even))
        def _():
            for order in range(2):
                begin(order, 0, 1)
                begin_other(order, 0)

        for order in range(2):
            begin(order, 2)
            begin_other(order, 1)
    with jax.named_scope("mate_own"):
        allow(MATE)
        for k in range(2):
            across(k, s, 0, D_EXPERT).start()

    def at_plane(table):
        return sum(jnp.where(z == k, v, 0) for k, v in enumerate(table) if v) + jnp.where(z < 0, 1, 0)

    left = [at_plane(LEFT[lane]) for lane in range(2)]
    taken = [at_plane([LEFT[lane][(k + 4) % Z] for k in range(Z)]) for lane in range(2)]

    odd = jnp.logical_not(even)

    def own_arrived(i):
        with jax.named_scope(f"half_a{i}"):
            start, length = chunks(*GROUPS[i])
            arrived(length, first_recv.at[i])
            for lane in range(2):
                shard = arriving(lane, 1)
                for j in range(MOST):
                    if start <= j * STEP < start + length:
                        @pl.when(j >= left[lane])
                        def _():
                            shared(lane, j, shard, lanes[lane]).start()
                for p, (lo, n) in enumerate(PASSED):
                    if start <= lo < start + length:
                        if p == LAST:
                            again = copy(lane, shard, lo, n, (FORE_MATE, BACK_MATE)[lane], ici_send, passed_recv.at[LAST + 1])
                            more = z == (7, 3)[lane]

                            @pl.when(jnp.logical_and(more, c == 0))
                            def _():
                                again.start()

                            passed(lane, p, shard).start()

                            @pl.when(jnp.logical_and(more, c == 1))
                            def _():
                                again.start()
                        else:
                            passed(lane, p, shard).start()
                across(lane, shard, start, length).start()

    def other_arrived(i):
        with jax.named_scope(f"half_b{i}"):
            start, length = chunks(*OTHER[i])
            arrived(length, second_recv.at[i])
            for lane in range(2):
                for j in range(MOST):
                    if start <= j * STEP < start + length and max(LEFT[lane]) > j:
                        @pl.when(j < taken[lane])
                        def _():
                            shared(lane, j, arriving(1 - lane, 1), lanes[1 - lane]).start()
            for lane in range(2):
                across(1 - lane, arriving(lane, 1), start, length).start()

    def router_rest():
        with jax.named_scope("router_x1"):
            landed(ring.at[c, y, x, 0:5], 1)
            post(row(0), XP, 2).start()
            post(row(0), XM, 2).start()
        with jax.named_scope("router_x2"):
            landed(ring.at[c, y, 0:2], 2)
            post(row(-1), XP, 3).start()
        with jax.named_scope("router_y1"):
            landed(ring.at[c, y, 0], 3)
            post(plane(0), YP, 4).start()
            post(plane(0), YM, 4).start()
        for i in range(3):
            with jax.named_scope(f"router_y{i + 2}"):
                landed(ring.at[c, 0:2], 4 + i)
                post(plane(-1 - i), YP, 5 + i).start()
                if i < 2:
                    post(plane(1 + i), YM, 5 + i).start()
        with jax.named_scope("router_mate"):
            landed(ring.at[c, 0], 7)
            post(ring.at[c], MATE, 8).start()

    def arrivals():
        own_arrived(0)
        own_arrived(1)
        other_arrived(0)
        own_arrived(2)

    @pl.when(even)
    def _():
        arrivals()
        router_rest()
        other_arrived(1)

    @pl.when(jnp.logical_not(even))
    def _():
        router_rest()
        arrivals()
        other_arrived(1)

    with jax.named_scope("router_end"):
        landed(ring.at[1 - c], 8)

        def lay(i, _):
            yy, xx = i >> 2, i & (X - 1)
            for zz in range(Z):
                for cc in range(2):
                    lo = (2 * (zz // 2) + cc) * WIDE
                    flat[pl.ds((zz % 2) * (Y * X) + i, 1), lo : lo + WIDE] = ring[cc, yy, xx, zz]
            return 0

        lax.fori_loop(0, Y * X, lay, 0)
        router[...] = flat[...].astype(jnp.bfloat16)
    def passed_across(lo, n):
        for lane in range(2):
            across(lane, arriving(lane, 2), lo, n).start()

    with jax.named_scope("shared"):
        arrived(MOST * STEP, passed_recv.at[LAST + 2])
        passed_across(0, MOST * STEP)
    for p, (lo, n) in enumerate(PASSED):
        with jax.named_scope(f"passed{p}"):
            arrived(n, passed_recv.at[p])
            if p < LAST:
                passed_across(lo, n)

    with jax.named_scope("finish"):
        twice = z == 1

        @pl.when(jnp.logical_not(twice))
        def _():
            passed_across(*PASSED[LAST])

        def rows_sent(k):
            shared_rows = STEP * (2 * MOST + sum(LEFT[lane][(k + 4) % Z] - LEFT[lane][k] for lane in range(2)))
            return 4 * D_EXPERT + 2 * (D_EXPERT - MOST * STEP) + shared_rows + TWICE * (k in (3, 7))

        for n in sorted({rows_sent(k) for k in range(Z)}):
            @pl.when(at_plane([int(rows_sent(k) == n) for k in range(Z)]) > 0)
            def _():
                sent(gate.at[0 : n // SHARDS, :], ici_send)
        sent(ring.at[c, y, x, 0:7], r_send.at[0])
        sent(held.at[0, 0:168, 0:768], r_send.at[1])

        def swapped(ref):
            sent(ref, core_sem.at[0])
            pltpu.make_async_remote_copy(ref, ref, core_sem.at[0], core_sem.at[1], device_id=near[MATE], device_id_type=MESH).wait_recv()

        @pl.when(twice)
        def _():
            arrived(TWICE, passed_recv.at[LAST + 1])
            swapped(gate.at[0 : D_EXPERT - 2 * TWICE // SHARDS, :])

        @pl.when(jnp.logical_not(twice))
        def _():
            swapped(gate)


def store(gate, up, router, gate_out, up_out, router_out, sem):
    copies = [pltpu.make_async_copy(a, b, sem.at[i])
              for i, (a, b) in enumerate(((gate, gate_out), (up, up_out), (router, router_out)))]
    for copy in copies:
        copy.start()
    for copy in copies:
        copy.wait()


def local(w_gate, avg_gate, w_up, avg_up, mix_share, router_weight, router_gain):
    out = jax.ShapeDtypeStruct((D_EXPERT, D_MODEL), jnp.bfloat16)
    outs = (out, out, jax.ShapeDtypeStruct((EXPERTS, D_MODEL), jnp.bfloat16))
    hbm = pl.BlockSpec(memory_space=pltpu.HBM)
    vmem = pl.BlockSpec(memory_space=pltpu.VMEM)
    dma = pltpu.SemaphoreType.DMA
    gathered = pl.pallas_call(
        kernel,
        out_shape=outs,
        in_specs=[hbm] * 6 + [vmem],
        out_specs=(vmem,) * 3,
        scratch_shapes=[
            pltpu.VMEM((4, WIDE, D_EXPERT), jnp.float32),
            dma((len(GROUPS),)),
            pltpu.VMEM((2, 1, WIDE), jnp.float32),
            dma,
            pltpu.VMEM((2, Y, X, Z, 1, WIDE), jnp.float32),
            pltpu.VMEM((EXPERTS, D_MODEL), jnp.float32),
            pltpu.SemaphoreType.REGULAR((4,)),
            dma((len(GROUPS),)),
            dma((len(OTHER),)),
            dma((len(PASSED) + 2,)),
            dma,
            dma((2,)),
            dma((2,)),
            dma((9,)),
        ],
        compiler_params=pltpu.CompilerParams(
            collective_id=0, has_side_effects=True, vmem_limit_bytes=40 * 2**20),
        name="mix_and_gather",
    )(*(pltpu.with_memory_space_constraint(a, pltpu.HBM) for a in (
        w_gate, avg_gate, w_up, avg_up, router_weight.reshape(1, WIDE), router_gain.reshape(1, WIDE))),
      mix_share.reshape(1, 1))
    gate, up, router = pl.pallas_call(
        store,
        out_shape=outs,
        in_specs=[vmem] * 3,
        out_specs=(hbm,) * 3,
        scratch_shapes=[dma((3,))],
        compiler_params=pltpu.CompilerParams(vmem_limit_bytes=2**20),
        name="store",
    )(*gathered)
    return gate[None], up[None], router.T


def solution(mesh):
    return jax.shard_map(
        local,
        mesh=mesh,
        in_specs=(
            P("expert", "shard", None),
            P("expert", "shard", None),
            P("expert", "shard", None),
            P("expert", "shard", None),
            P("expert"),
            P("shard", "expert"),
            P("shard"),
        ),
        out_specs=(P("expert", None, None), P("expert", None, None), P()),
        check_vma=False,
    )
```

```python
import jax
import jax.numpy as jnp
from jax import lax
from jax.experimental import pallas as pl
from jax.experimental.pallas import tpu as pltpu
from jax.sharding import PartitionSpec as P

MESH = pl.DeviceIdType.MESH
D_MODEL, D_EXPERT, EXPERTS, SHARDS = 2048, 1024, 64, 8
WIDE = D_MODEL // SHARDS
ROWS = 128
CHUNKS = D_EXPERT // ROWS
X, Y, Z = 4, 8, 8
FORE, BACK, MATE, ZP, ZM, XP, XM, YP, YM, FORE_MATE, BACK_MATE = range(11)
OPPOSITE = (BACK, FORE, MATE, ZM, ZP, XM, XP, YM, YP, BACK_MATE, FORE_MATE)
TWICE = 64
GROUPS = ((0, 1), (1, 3), (4, 4))
OTHER = ((0, 2), (2, 6))
STEP, MOST = 64, 4
PASSED = ((MOST * STEP, 256), (512, 256), (768, 128), (896, 128 - TWICE), (1024 - TWICE, TWICE))
LAST = len(PASSED) - 1
LEFT = (0, 0, 0, 0, 0, 0, 4, 0), (3, 0, 0, 0, 2, 1, 0, 0)
LATE = 6


def kernel(wg, ag, wu, au, rw_any, gain_any, mix, gate, up, router, held, load_sem, small, small_sem, ring, flat,
           ready, first_recv, second_recv, passed_recv, ici_send, core_sem, r_send, r_recv):
    e, s = lax.axis_index("expert"), lax.axis_index("shard")
    x, y, z_lo = e & (X - 1), (e >> 2) & (Y - 1), e >> 5
    z_hi, c = s >> 1, s & 1
    z = 2 * z_hi + z_lo

    def columns_of(g):
        return pl.ds(GROUPS[g][0] * ROWS, GROUPS[g][1] * ROWS)

    for i, ref in enumerate((rw_any, gain_any)):
        pltpu.make_async_copy(ref, small.at[i], small_sem).start()
    for g in range(len(GROUPS)):
        for k in (1, 0):
            for i, ref in enumerate(((wg, ag), (wu, au))[k]):
                pltpu.make_async_copy(ref.at[0, :, columns_of(g)], held.at[2 * k + i, :, columns_of(g)], load_sem.at[g]).start()

    def loaded(g):
        ref = held.at[:, :, columns_of(g)]
        pltpu.make_async_copy(ref, ref, load_sem.at[g]).wait()

    def place(dx=0, dy=0, dz=0, dc=0):
        return (x + dx) & (X - 1), (y + dy) & (Y - 1), (z + dz) & (Z - 1), (c + dc) & 1

    def device(p):
        return {"expert": ((p[2] & 1) << 5) + (p[1] << 2) + p[0], "shard": (p[2] & 6) + p[3]}

    def rank(p):
        order = (p[2] << 7) + (p[1] << 4) + (p[0] << 2) + 2 - 2 * p[3]
        return jnp.where(order == 2, (LATE << 7) - 1, order)

    places = [place(dz=2), place(dz=-2), place(dc=1), place(dz=1), place(dz=-1), place(dx=1), place(dx=-1), place(dy=1), place(dy=-1),
              place(dz=2, dc=1), place(dz=-2, dc=1)]
    near = [device(p) for p in places]
    own_rank = rank(place())
    earlier = [rank(p) < own_rank for p in places]
    lanes = (FORE, BACK)

    barrier = pltpu.get_barrier_semaphore()
    for k in range(11):
        @pl.when(jnp.logical_not(earlier[k]))
        def _():
            pl.semaphore_signal(barrier, inc=1, device_id=near[k], device_id_type=MESH)
    def answer():
        before = sum(a.astype(jnp.int32) for a in earlier)

        @pl.when(before > 0)
        def _():
            pl.semaphore_wait(barrier, before)

        for k in range(11):
            @pl.when(earlier[k])
            def _():
                pl.semaphore_signal(ready.at[min(OPPOSITE[k], ZP)], inc=1, device_id=near[k], device_id_type=MESH)

    def allow(k):
        @pl.when(jnp.logical_not(earlier[k]))
        def _():
            pl.semaphore_wait(ready.at[k], 1)

    def allow_rest():
        after = sum(1 - earlier[k].astype(jnp.int32) for k in range(ZP, 11))

        @pl.when(after > 0)
        def _():
            pl.semaphore_wait(ready.at[ZP], after)

    share = mix[...]
    rest = 1.0 - share

    def columns(shard):
        return pl.ds(pl.multiple_of(shard * WIDE, WIDE), WIDE)

    def rows(j, n=1):
        return pl.ds(pl.multiple_of(j * ROWS, ROWS), n * ROWS)

    def compute(k, j):
        fresh = share * held[2 * k, :, rows(j)] + rest * held[2 * k + 1, :, rows(j)]
        (gate, up)[k][rows(j), columns(s)] = fresh.T.astype(jnp.bfloat16)

    def copy(k, shard, lo, n, to, send, recv):
        ref = (gate, up)[k].at[pl.ds(lo, n), columns(shard)]
        return pltpu.make_async_remote_copy(ref, ref, send, recv, device_id=near[to], device_id_type=MESH)

    def chunks(j, n):
        return j * ROWS, n * ROWS

    def first(lane, i):
        return copy(lane, s, *chunks(*GROUPS[i]), lanes[lane], ici_send, first_recv.at[i])

    def second(lane, i):
        return copy(1 - lane, s, *chunks(*OTHER[i]), lanes[lane], ici_send, second_recv.at[i])

    def passed(lane, p, shard):
        return copy(lane, shard, *PASSED[p], lanes[lane], ici_send, passed_recv.at[p])

    def shared(lane, i, shard, to):
        return copy(lane, shard, i * STEP, STEP, to, ici_send, passed_recv.at[LAST + 2])

    def across(k, shard, lo, n):
        return copy(k, shard, lo, n, MATE, core_sem.at[0], core_sem.at[1])

    def arrived(n, sem):
        ref = gate.at[0:n, 0 : 2 * WIDE]
        pltpu.make_async_remote_copy(ref, ref, core_sem.at[0], sem, device_id=near[MATE], device_id_type=MESH).wait_recv()

    def arriving(lane, far):
        return ((z_hi + (4 - far if lane == 0 else far)) & 3) * 2 + c

    def sent(ref, sem):
        pltpu.make_async_remote_copy(ref, ref, sem, core_sem.at[1], device_id=near[MATE], device_id_type=MESH).wait_send()

    def post(ref, to, i):
        return pltpu.make_async_remote_copy(
            ref, ref, r_send.at[min(i // 2, 1)], r_recv.at[i], device_id=near[to], device_id_type=MESH)

    def piece(k):
        return ring.at[c, y, x, (z + k) & (Z - 1)]

    def row(k):
        return ring.at[c, y, (x + k) & (X - 1)]

    def plane(k):
        return ring.at[c, (y + k) & (Y - 1)]

    def landed(ref, i):
        post(ref, MATE, i).wait_recv()

    even = (z & 1) == 0
    zeroth = jnp.logical_or(z < 2, z >= 6)

    def in_turn(order, do):
        for lane in range(2):
            @pl.when(zeroth if lane == order else jnp.logical_not(zeroth))
            def _():
                do(lane)

    def own_piece(lane):
        post(piece(0), lanes[lane], 0).start()

    def begin(order, *which):
        in_turn(order, lambda lane: [first(lane, i).start() for i in which])

    def begin_other(order, *which):
        in_turn(order, lambda lane: [second(lane, i).start() for i in which])

    both = jnp.logical_and(even, z >= 6)
    one = jnp.logical_and(even, z < 6)

    with jax.named_scope("first_chunk"):
        answer()
        loaded(0)
        compute(1, 0)
        compute(0, 0)
    with jax.named_scope("admit_first"):
        in_turn(0, lambda lane: allow(lanes[lane]))

        @pl.when(even)
        def _():
            begin(0, 0)

        @pl.when(both)
        def _():
            begin(1, 0)
    with jax.named_scope("compute"):
        def more(j, _):
            for k in (1, 0):
                compute(k, j)
            return 0

        def more_of(g):
            loaded(g)
            lax.fori_loop(GROUPS[g][0], sum(GROUPS[g]), more, 0)

        more_of(1)
        pltpu.make_async_copy(small, small, small_sem).wait()
        ring[c, y, x, z] = small[0] * small[1]
        in_turn(0, own_piece)

        @pl.when(even)
        def _():
            begin(0, 1)

        @pl.when(both)
        def _():
            in_turn(1, own_piece)
            begin(1, 1)

        @pl.when(even)
        def _():
            begin_other(0, 0)

        more_of(2)
    with jax.named_scope("admit_second"):
        in_turn(1, lambda lane: allow(lanes[lane]))

        @pl.when(jnp.logical_not(both))
        def _():
            in_turn(1, own_piece)

        @pl.when(one)
        def _():
            begin(1, 0, 1)

        @pl.when(even)
        def _():
            begin_other(1, 0)
    with jax.named_scope("z_steps"):
        allow_rest()
        post(piece(0), ZP, 1).start()
        post(piece(0), ZM, 1).start()
        landed(ring.at[c, y, x, 0:2], 0)
        post(piece(-2), ZP, 1).start()
        post(piece(2), ZM, 1).start()
        post(piece(-2), FORE, 1).start()
    with jax.named_scope("own"):
        @pl.when(jnp.logical_not(even))
        def _():
            for order in range(2):
                begin(order, 0, 1)
                begin_other(order, 0)

        for order in range(2):
            begin(order, 2)
            begin_other(order, 1)
    with jax.named_scope("mate_own"):
        allow(MATE)
        for k in range(2):
            across(k, s, 0, D_EXPERT).start()

    def at_plane(table):
        return sum(jnp.where(z == k, v, 0) for k, v in enumerate(table) if v) + jnp.where(z < 0, 1, 0)

    left = [at_plane(LEFT[lane]) for lane in range(2)]
    taken = [at_plane([LEFT[lane][(k + 4) % Z] for k in range(Z)]) for lane in range(2)]

    odd = jnp.logical_not(even)

    def own_arrived(i):
        with jax.named_scope(f"half_a{i}"):
            start, length = chunks(*GROUPS[i])
            arrived(length, first_recv.at[i])
            for lane in range(2):
                shard = arriving(lane, 1)
                for j in range(MOST):
                    if start <= j * STEP < start + length:
                        @pl.when(j >= left[lane])
                        def _():
                            shared(lane, j, shard, lanes[lane]).start()
                for p, (lo, n) in enumerate(PASSED):
                    if start <= lo < start + length:
                        if p == LAST:
                            again = copy(lane, shard, lo, n, (FORE_MATE, BACK_MATE)[lane], ici_send, passed_recv.at[LAST + 1])
                            more = z == (7, 3)[lane]

                            @pl.when(jnp.logical_and(more, c == 0))
                            def _():
                                again.start()

                            passed(lane, p, shard).start()

                            @pl.when(jnp.logical_and(more, c == 1))
                            def _():
                                again.start()
                        else:
                            passed(lane, p, shard).start()
                across(lane, shard, start, length).start()

    def other_arrived(i):
        with jax.named_scope(f"half_b{i}"):
            start, length = chunks(*OTHER[i])
            arrived(length, second_recv.at[i])
            for lane in range(2):
                for j in range(MOST):
                    if start <= j * STEP < start + length and max(LEFT[lane]) > j:
                        @pl.when(j < taken[lane])
                        def _():
                            shared(lane, j, arriving(1 - lane, 1), lanes[1 - lane]).start()
            for lane in range(2):
                across(1 - lane, arriving(lane, 1), start, length).start()

    def router_rest():
        with jax.named_scope("router_x1"):
            landed(ring.at[c, y, x, 0:5], 1)
            post(row(0), XP, 2).start()
            post(row(0), XM, 2).start()
        with jax.named_scope("router_x2"):
            landed(ring.at[c, y, 0:2], 2)
            post(row(-1), XP, 3).start()
        with jax.named_scope("router_y1"):
            landed(ring.at[c, y, 0], 3)
            post(plane(0), YP, 4).start()
            post(plane(0), YM, 4).start()
        for i in range(3):
            with jax.named_scope(f"router_y{i + 2}"):
                landed(ring.at[c, 0:2], 4 + i)
                post(plane(-1 - i), YP, 5 + i).start()
                if i < 2:
                    post(plane(1 + i), YM, 5 + i).start()
        with jax.named_scope("router_mate"):
            landed(ring.at[c, 0], 7)
            post(ring.at[c], MATE, 8).start()

    def arrivals():
        own_arrived(0)
        own_arrived(1)
        other_arrived(0)
        own_arrived(2)

    @pl.when(even)
    def _():
        arrivals()
        router_rest()
        other_arrived(1)

    @pl.when(jnp.logical_not(even))
    def _():
        router_rest()
        arrivals()
        other_arrived(1)

    with jax.named_scope("router_end"):
        landed(ring.at[1 - c], 8)

        def lay(i, _):
            yy, xx = i >> 2, i & (X - 1)
            for zz in range(Z):
                for cc in range(2):
                    lo = (2 * (zz // 2) + cc) * WIDE
                    flat[pl.ds((zz % 2) * (Y * X) + i, 1), lo : lo + WIDE] = ring[cc, yy, xx, zz]
            return 0

        lax.fori_loop(0, Y * X, lay, 0)
        router[...] = flat[...].astype(jnp.bfloat16)
    def passed_across(lo, n):
        for lane in range(2):
            across(lane, arriving(lane, 2), lo, n).start()

    with jax.named_scope("shared"):
        arrived(MOST * STEP, passed_recv.at[LAST + 2])
        passed_across(0, MOST * STEP)
    for p, (lo, n) in enumerate(PASSED[:LAST]):
        with jax.named_scope(f"passed{p}"):
            arrived(n, passed_recv.at[p])
            passed_across(lo, n)

    with jax.named_scope("finish"):
        def rows_sent(k):
            shared_rows = STEP * (2 * MOST + sum(LEFT[lane][(k + 4) % Z] - LEFT[lane][k] for lane in range(2)))
            return 4 * D_EXPERT + 2 * (D_EXPERT - MOST * STEP) + shared_rows + TWICE * (k in (3, 7))

        sent(ring.at[c, y, x, 0:7], r_send.at[0])
        sent(held.at[0, 0:168, 0:768], r_send.at[1])
        twice = z == 1

        @pl.when(twice)
        def _():
            sent(gate.at[0 : rows_sent(1) // SHARDS, :], ici_send)

        arrived(TWICE, passed_recv.at[LAST])

        @pl.when(jnp.logical_not(twice))
        def _():
            passed_across(*PASSED[LAST])

        for n in sorted({rows_sent(k) for k in range(Z) if k != 1}):
            @pl.when(at_plane([int(k != 1 and rows_sent(k) == n) for k in range(Z)]) > 0)
            def _():
                sent(gate.at[0 : n // SHARDS, :], ici_send)

        def swapped(ref):
            sent(ref, core_sem.at[0])
            pltpu.make_async_remote_copy(ref, ref, core_sem.at[0], core_sem.at[1], device_id=near[MATE], device_id_type=MESH).wait_recv()

        @pl.when(twice)
        def _():
            arrived(TWICE, passed_recv.at[LAST + 1])
            swapped(gate.at[0 : D_EXPERT - 2 * TWICE // SHARDS, :])

        @pl.when(jnp.logical_not(twice))
        def _():
            swapped(gate)


def store(gate, up, router, gate_out, up_out, router_out, sem):
    copies = [pltpu.make_async_copy(a, b, sem.at[i])
              for i, (a, b) in enumerate(((gate, gate_out), (up, up_out), (router, router_out)))]
    for copy in copies:
        copy.start()
    for copy in copies:
        copy.wait()


def local(w_gate, avg_gate, w_up, avg_up, mix_share, router_weight, router_gain):
    out = jax.ShapeDtypeStruct((D_EXPERT, D_MODEL), jnp.bfloat16)
    outs = (out, out, jax.ShapeDtypeStruct((EXPERTS, D_MODEL), jnp.bfloat16))
    hbm = pl.BlockSpec(memory_space=pltpu.HBM)
    vmem = pl.BlockSpec(memory_space=pltpu.VMEM)
    dma = pltpu.SemaphoreType.DMA
    gathered = pl.pallas_call(
        kernel,
        out_shape=outs,
        in_specs=[hbm] * 6 + [vmem],
        out_specs=(vmem,) * 3,
        scratch_shapes=[
            pltpu.VMEM((4, WIDE, D_EXPERT), jnp.float32),
            dma((len(GROUPS),)),
            pltpu.VMEM((2, 1, WIDE), jnp.float32),
            dma,
            pltpu.VMEM((2, Y, X, Z, 1, WIDE), jnp.float32),
            pltpu.VMEM((EXPERTS, D_MODEL), jnp.float32),
            pltpu.SemaphoreType.REGULAR((4,)),
            dma((len(GROUPS),)),
            dma((len(OTHER),)),
            dma((len(PASSED) + 2,)),
            dma,
            dma((2,)),
            dma((2,)),
            dma((9,)),
        ],
        compiler_params=pltpu.CompilerParams(
            collective_id=0, has_side_effects=True, vmem_limit_bytes=40 * 2**20),
        name="mix_and_gather",
    )(*(pltpu.with_memory_space_constraint(a, pltpu.HBM) for a in (
        w_gate, avg_gate, w_up, avg_up, router_weight.reshape(1, WIDE), router_gain.reshape(1, WIDE))),
      mix_share.reshape(1, 1))
    gate, up, router = pl.pallas_call(
        store,
        out_shape=outs,
        in_specs=[vmem] * 3,
        out_specs=(hbm,) * 3,
        scratch_shapes=[dma((3,))],
        compiler_params=pltpu.CompilerParams(vmem_limit_bytes=2**20),
        name="store",
    )(*gathered)
    return gate[None], up[None], router.T


def solution(mesh):
    return jax.shard_map(
        local,
        mesh=mesh,
        in_specs=(
            P("expert", "shard", None),
            P("expert", "shard", None),
            P("expert", "shard", None),
            P("expert", "shard", None),
            P("expert"),
            P("shard", "expert"),
            P("shard"),
        ),
        out_specs=(P("expert", None, None), P("expert", None, None), P()),
        check_vma=False,
    )
```

```python
import jax
import jax.numpy as jnp
from jax import lax
from jax.experimental import pallas as pl
from jax.experimental.pallas import tpu as pltpu
from jax.sharding import PartitionSpec as P

MESH = pl.DeviceIdType.MESH
D_MODEL, D_EXPERT, EXPERTS, SHARDS = 2048, 1024, 64, 8
WIDE = D_MODEL // SHARDS
ROWS = 128
CHUNKS = D_EXPERT // ROWS
X, Y, Z = 4, 8, 8
FORE, BACK, MATE, ZP, ZM, XP, XM, YP, YM, FORE_MATE, BACK_MATE = range(11)
OPPOSITE = (BACK, FORE, MATE, ZM, ZP, XM, XP, YM, YP, BACK_MATE, FORE_MATE)
TWICE = 64
GROUPS = ((0, 1), (1, 3), (4, 4))
OTHER = ((0, 2), (2, 6))
STEP, MOST = 64, 4
PASSED = ((MOST * STEP, 256), (512, 256), (768, 128), (896, 128 - TWICE), (1024 - TWICE, TWICE))
LAST = len(PASSED) - 1
LEFT = (0, 0, 0, 0, 0, 0, 4, 0), (3, 0, 0, 0, 2, 1, 0, 0)
LATE = 6


def kernel(wg, ag, wu, au, rw_any, gain_any, mix, gate, up, router, held, load_sem, small, small_sem, ring, flat,
           ready, first_recv, second_recv, passed_recv, ici_send, core_sem, r_send, r_recv):
    e, s = lax.axis_index("expert"), lax.axis_index("shard")
    x, y, z_lo = e & (X - 1), (e >> 2) & (Y - 1), e >> 5
    z_hi, c = s >> 1, s & 1
    z = 2 * z_hi + z_lo

    def columns_of(g):
        return pl.ds(GROUPS[g][0] * ROWS, GROUPS[g][1] * ROWS)

    for i, ref in enumerate((rw_any, gain_any)):
        pltpu.make_async_copy(ref, small.at[i], small_sem).start()
    for g in range(len(GROUPS)):
        for k in (1, 0):
            for i, ref in enumerate(((wg, ag), (wu, au))[k]):
                pltpu.make_async_copy(ref.at[0, :, columns_of(g)], held.at[2 * k + i, :, columns_of(g)], load_sem.at[g]).start()

    def loaded(g):
        ref = held.at[:, :, columns_of(g)]
        pltpu.make_async_copy(ref, ref, load_sem.at[g]).wait()

    def place(dx=0, dy=0, dz=0, dc=0):
        return (x + dx) & (X - 1), (y + dy) & (Y - 1), (z + dz) & (Z - 1), (c + dc) & 1

    def device(p):
        return {"expert": ((p[2] & 1) << 5) + (p[1] << 2) + p[0], "shard": (p[2] & 6) + p[3]}

    def rank(p):
        order = (p[2] << 7) + (p[1] << 4) + (p[0] << 2) + 2 - 2 * p[3]
        return jnp.where(order == 2, (LATE << 7) - 1, order)

    places = [place(dz=2), place(dz=-2), place(dc=1), place(dz=1), place(dz=-1), place(dx=1), place(dx=-1), place(dy=1), place(dy=-1),
              place(dz=2, dc=1), place(dz=-2, dc=1)]
    near = [device(p) for p in places]
    own_rank = rank(place())
    earlier = [rank(p) < own_rank for p in places]
    lanes = (FORE, BACK)

    barrier = pltpu.get_barrier_semaphore()
    for k in range(11):
        @pl.when(jnp.logical_not(earlier[k]))
        def _():
            pl.semaphore_signal(barrier, inc=1, device_id=near[k], device_id_type=MESH)
    def answer():
        before = sum(a.astype(jnp.int32) for a in earlier)

        @pl.when(before > 0)
        def _():
            pl.semaphore_wait(barrier, before)

        for k in range(11):
            @pl.when(earlier[k])
            def _():
                pl.semaphore_signal(ready.at[min(OPPOSITE[k], ZP)], inc=1, device_id=near[k], device_id_type=MESH)

    def allow(k):
        @pl.when(jnp.logical_not(earlier[k]))
        def _():
            pl.semaphore_wait(ready.at[k], 1)

    def allow_rest():
        after = sum(1 - earlier[k].astype(jnp.int32) for k in range(ZP, 11))

        @pl.when(after > 0)
        def _():
            pl.semaphore_wait(ready.at[ZP], after)

    share = mix[...]
    rest = 1.0 - share

    def columns(shard):
        return pl.ds(pl.multiple_of(shard * WIDE, WIDE), WIDE)

    def rows(j, n=1):
        return pl.ds(pl.multiple_of(j * ROWS, ROWS), n * ROWS)

    def compute(k, j):
        fresh = share * held[2 * k, :, rows(j)] + rest * held[2 * k + 1, :, rows(j)]
        (gate, up)[k][rows(j), columns(s)] = fresh.T.astype(jnp.bfloat16)

    def copy(k, shard, lo, n, to, send, recv):
        ref = (gate, up)[k].at[pl.ds(lo, n), columns(shard)]
        return pltpu.make_async_remote_copy(ref, ref, send, recv, device_id=near[to], device_id_type=MESH)

    def chunks(j, n):
        return j * ROWS, n * ROWS

    def first(lane, i):
        return copy(lane, s, *chunks(*GROUPS[i]), lanes[lane], ici_send, first_recv.at[i])

    def second(lane, i):
        return copy(1 - lane, s, *chunks(*OTHER[i]), lanes[lane], ici_send, second_recv.at[i])

    def passed(lane, p, shard):
        return copy(lane, shard, *PASSED[p], lanes[lane], ici_send, passed_recv.at[max(p - 1, 0)])

    def shared(lane, i, shard, to):
        return copy(lane, shard, i * STEP, STEP, to, ici_send, passed_recv.at[0])

    def across(k, shard, lo, n):
        return copy(k, shard, lo, n, MATE, core_sem.at[0], core_sem.at[1])

    def arrived(n, sem):
        ref = gate.at[0:n, 0 : 2 * WIDE]
        pltpu.make_async_remote_copy(ref, ref, core_sem.at[0], sem, device_id=near[MATE], device_id_type=MESH).wait_recv()

    def arriving(lane, far):
        return ((z_hi + (4 - far if lane == 0 else far)) & 3) * 2 + c

    def sent(ref, sem):
        pltpu.make_async_remote_copy(ref, ref, sem, core_sem.at[1], device_id=near[MATE], device_id_type=MESH).wait_send()

    def post(ref, to, i):
        return pltpu.make_async_remote_copy(
            ref, ref, r_send.at[min(i // 2, 1)], r_recv.at[i], device_id=near[to], device_id_type=MESH)

    def piece(k):
        return ring.at[c, y, x, (z + k) & (Z - 1)]

    def row(k):
        return ring.at[c, y, (x + k) & (X - 1)]

    def plane(k):
        return ring.at[c, (y + k) & (Y - 1)]

    def landed(ref, i):
        post(ref, MATE, i).wait_recv()

    even = (z & 1) == 0
    zeroth = jnp.logical_or(z < 2, z >= 6)

    def in_turn(order, do):
        for lane in range(2):
            @pl.when(zeroth if lane == order else jnp.logical_not(zeroth))
            def _():
                do(lane)

    def own_piece(lane):
        post(piece(0), lanes[lane], 0).start()

    def begin(order, *which):
        in_turn(order, lambda lane: [first(lane, i).start() for i in which])

    def begin_other(order, *which):
        in_turn(order, lambda lane: [second(lane, i).start() for i in which])

    both = jnp.logical_and(even, z >= 6)
    one = jnp.logical_and(even, z < 6)

    with jax.named_scope("first_chunk"):
        answer()
        loaded(0)
        compute(1, 0)
        compute(0, 0)
    with jax.named_scope("admit_first"):
        in_turn(0, lambda lane: allow(lanes[lane]))

        @pl.when(even)
        def _():
            begin(0, 0)

        @pl.when(both)
        def _():
            begin(1, 0)
    with jax.named_scope("compute"):
        def more(j, _):
            for k in (1, 0):
                compute(k, j)
            return 0

        def more_of(g):
            loaded(g)
            lax.fori_loop(GROUPS[g][0], sum(GROUPS[g]), more, 0)

        more_of(1)
        pltpu.make_async_copy(small, small, small_sem).wait()
        ring[c, y, x, z] = small[0] * small[1]
        in_turn(0, own_piece)

        @pl.when(even)
        def _():
            begin(0, 1)

        @pl.when(both)
        def _():
            in_turn(1, own_piece)
            begin(1, 1)

        @pl.when(even)
        def _():
            begin_other(0, 0)

        more_of(2)
    with jax.named_scope("admit_second"):
        in_turn(1, lambda lane: allow(lanes[lane]))

        @pl.when(jnp.logical_not(both))
        def _():
            in_turn(1, own_piece)

        @pl.when(one)
        def _():
            begin(1, 0, 1)

        @pl.when(even)
        def _():
            begin_other(1, 0)
    with jax.named_scope("z_steps"):
        allow_rest()
        post(piece(0), ZP, 1).start()
        post(piece(0), ZM, 1).start()
        landed(ring.at[c, y, x, 0:2], 0)
        post(piece(-2), ZP, 1).start()
        post(piece(2), ZM, 1).start()
        post(piece(-2), FORE, 1).start()
    with jax.named_scope("own"):
        @pl.when(jnp.logical_not(even))
        def _():
            for order in range(2):
                begin(order, 0, 1)
                begin_other(order, 0)

        for order in range(2):
            begin(order, 2)
            begin_other(order, 1)
    with jax.named_scope("mate_own"):
        allow(MATE)
        for k in range(2):
            across(k, s, 0, D_EXPERT).start()

    def at_plane(table):
        return sum(jnp.where(z == k, v, 0) for k, v in enumerate(table) if v) + jnp.where(z < 0, 1, 0)

    left = [at_plane(LEFT[lane]) for lane in range(2)]
    taken = [at_plane([LEFT[lane][(k + 4) % Z] for k in range(Z)]) for lane in range(2)]

    odd = jnp.logical_not(even)

    def own_arrived(i):
        with jax.named_scope(f"half_a{i}"):
            start, length = chunks(*GROUPS[i])
            arrived(length, first_recv.at[i])
            for lane in range(2):
                shard = arriving(lane, 1)
                for j in range(MOST):
                    if start <= j * STEP < start + length:
                        @pl.when(j >= left[lane])
                        def _():
                            shared(lane, j, shard, lanes[lane]).start()
                for p, (lo, n) in enumerate(PASSED):
                    if start <= lo < start + length:
                        if p == LAST:
                            again = copy(lane, shard, lo, n, (FORE_MATE, BACK_MATE)[lane], ici_send, passed_recv.at[LAST])
                            more = z == (7, 3)[lane]

                            @pl.when(jnp.logical_and(more, c == 0))
                            def _():
                                again.start()

                            passed(lane, p, shard).start()

                            @pl.when(jnp.logical_and(more, c == 1))
                            def _():
                                again.start()
                        else:
                            passed(lane, p, shard).start()
                across(lane, shard, start, length).start()

    def other_arrived(i):
        with jax.named_scope(f"half_b{i}"):
            start, length = chunks(*OTHER[i])
            arrived(length, second_recv.at[i])
            for lane in range(2):
                for j in range(MOST):
                    if start <= j * STEP < start + length and max(LEFT[lane]) > j:
                        @pl.when(j < taken[lane])
                        def _():
                            shared(lane, j, arriving(1 - lane, 1), lanes[1 - lane]).start()
            for lane in range(2):
                across(1 - lane, arriving(lane, 1), start, length).start()

    def router_rest():
        with jax.named_scope("router_x1"):
            landed(ring.at[c, y, x, 0:5], 1)
            post(row(0), XP, 2).start()
            post(row(0), XM, 2).start()
        with jax.named_scope("router_x2"):
            landed(ring.at[c, y, 0:2], 2)
            post(row(-1), XP, 3).start()
        with jax.named_scope("router_y1"):
            landed(ring.at[c, y, 0], 3)
            post(plane(0), YP, 4).start()
            post(plane(0), YM, 4).start()
        for i in range(3):
            with jax.named_scope(f"router_y{i + 2}"):
                landed(ring.at[c, 0:2], 4 + i)
                post(plane(-1 - i), YP, 5 + i).start()
                if i < 2:
                    post(plane(1 + i), YM, 5 + i).start()
        with jax.named_scope("router_mate"):
            landed(ring.at[c, 0], 7)
            post(ring.at[c], MATE, 8).start()

    def arrivals():
        own_arrived(0)
        own_arrived(1)
        other_arrived(0)
        own_arrived(2)

    @pl.when(even)
    def _():
        arrivals()
        router_rest()
        other_arrived(1)

    @pl.when(jnp.logical_not(even))
    def _():
        router_rest()
        arrivals()
        other_arrived(1)

    with jax.named_scope("router_end"):
        landed(ring.at[1 - c], 8)

        def lay(i, _):
            yy, xx = i >> 2, i & (X - 1)
            for zz in range(Z):
                for cc in range(2):
                    lo = (2 * (zz // 2) + cc) * WIDE
                    flat[pl.ds((zz % 2) * (Y * X) + i, 1), lo : lo + WIDE] = ring[cc, yy, xx, zz]
            return 0

        lax.fori_loop(0, Y * X, lay, 0)
        router[...] = flat[...].astype(jnp.bfloat16)
    def passed_across(lo, n):
        for lane in range(2):
            across(lane, arriving(lane, 2), lo, n).start()

    with jax.named_scope("shared"):
        arrived(sum(PASSED[1]), passed_recv.at[0])
        passed_across(0, sum(PASSED[1]))
    for p, (lo, n) in enumerate(PASSED[:LAST]):
        if p > 1:
            with jax.named_scope(f"passed{p}"):
                arrived(n, passed_recv.at[p - 1])
                passed_across(lo, n)

    with jax.named_scope("finish"):
        def rows_sent(k):
            shared_rows = STEP * (2 * MOST + sum(LEFT[lane][(k + 4) % Z] - LEFT[lane][k] for lane in range(2)))
            return 4 * D_EXPERT + 2 * (D_EXPERT - MOST * STEP) + shared_rows + TWICE * (k in (3, 7))

        sent(ring.at[c, y, x, 0:7], r_send.at[0])
        sent(held.at[0, 0:168, 0:768], r_send.at[1])
        twice = z == 1

        @pl.when(twice)
        def _():
            sent(gate.at[0 : rows_sent(1) // SHARDS, :], ici_send)

        arrived(TWICE, passed_recv.at[LAST - 1])

        @pl.when(jnp.logical_not(twice))
        def _():
            passed_across(*PASSED[LAST])

        for n in sorted({rows_sent(k) for k in range(Z) if k != 1}):
            @pl.when(at_plane([int(k != 1 and rows_sent(k) == n) for k in range(Z)]) > 0)
            def _():
                sent(gate.at[0 : n // SHARDS, :], ici_send)

        def swapped(ref):
            sent(ref, core_sem.at[0])
            pltpu.make_async_remote_copy(ref, ref, core_sem.at[0], core_sem.at[1], device_id=near[MATE], device_id_type=MESH).wait_recv()

        @pl.when(twice)
        def _():
            arrived(TWICE, passed_recv.at[LAST])
            swapped(gate.at[0 : D_EXPERT - 2 * TWICE // SHARDS, :])

        @pl.when(jnp.logical_not(twice))
        def _():
            swapped(gate)


def store(gate, up, router, gate_out, up_out, router_out, sem):
    copies = [pltpu.make_async_copy(a, b, sem.at[i])
              for i, (a, b) in enumerate(((gate, gate_out), (up, up_out), (router, router_out)))]
    for copy in copies:
        copy.start()
    for copy in copies:
        copy.wait()


def local(w_gate, avg_gate, w_up, avg_up, mix_share, router_weight, router_gain):
    out = jax.ShapeDtypeStruct((D_EXPERT, D_MODEL), jnp.bfloat16)
    outs = (out, out, jax.ShapeDtypeStruct((EXPERTS, D_MODEL), jnp.bfloat16))
    hbm = pl.BlockSpec(memory_space=pltpu.HBM)
    vmem = pl.BlockSpec(memory_space=pltpu.VMEM)
    dma = pltpu.SemaphoreType.DMA
    gathered = pl.pallas_call(
        kernel,
        out_shape=outs,
        in_specs=[hbm] * 6 + [vmem],
        out_specs=(vmem,) * 3,
        scratch_shapes=[
            pltpu.VMEM((4, WIDE, D_EXPERT), jnp.float32),
            dma((len(GROUPS),)),
            pltpu.VMEM((2, 1, WIDE), jnp.float32),
            dma,
            pltpu.VMEM((2, Y, X, Z, 1, WIDE), jnp.float32),
            pltpu.VMEM((EXPERTS, D_MODEL), jnp.float32),
            pltpu.SemaphoreType.REGULAR((4,)),
            dma((len(GROUPS),)),
            dma((len(OTHER),)),
            dma((len(PASSED),)),
            dma,
            dma((2,)),
            dma((2,)),
            dma((9,)),
        ],
        compiler_params=pltpu.CompilerParams(
            collective_id=0, has_side_effects=True, vmem_limit_bytes=40 * 2**20),
        name="mix_and_gather",
    )(*(pltpu.with_memory_space_constraint(a, pltpu.HBM) for a in (
        w_gate, avg_gate, w_up, avg_up, router_weight.reshape(1, WIDE), router_gain.reshape(1, WIDE))),
      mix_share.reshape(1, 1))
    gate, up, router = pl.pallas_call(
        store,
        out_shape=outs,
        in_specs=[vmem] * 3,
        out_specs=(hbm,) * 3,
        scratch_shapes=[dma((3,))],
        compiler_params=pltpu.CompilerParams(vmem_limit_bytes=2**20),
        name="store",
    )(*gathered)
    return gate[None], up[None], router.T


def solution(mesh):
    return jax.shard_map(
        local,
        mesh=mesh,
        in_specs=(
            P("expert", "shard", None),
            P("expert", "shard", None),
            P("expert", "shard", None),
            P("expert", "shard", None),
            P("expert"),
            P("shard", "expert"),
            P("shard"),
        ),
        out_specs=(P("expert", None, None), P("expert", None, None), P()),
        check_vma=False,
    )
```

```python
import jax
import jax.numpy as jnp
from jax import lax
from jax.experimental import pallas as pl
from jax.experimental.pallas import tpu as pltpu
from jax.sharding import PartitionSpec as P

MESH = pl.DeviceIdType.MESH
D_MODEL, D_EXPERT, EXPERTS, SHARDS = 2048, 1024, 64, 8
WIDE = D_MODEL // SHARDS
ROWS = 128
CHUNKS = D_EXPERT // ROWS
X, Y, Z = 4, 8, 8
FORE, BACK, MATE, ZP, ZM, XP, XM, YP, YM, FORE_MATE, BACK_MATE = range(11)
OPPOSITE = (BACK, FORE, MATE, ZM, ZP, XM, XP, YM, YP, BACK_MATE, FORE_MATE)
TWICE = 64
GROUPS = ((0, 1), (1, 3), (4, 4))
OTHER = ((0, 2), (2, 6))
STEP, MOST = 64, 4
PASSED = ((MOST * STEP, 256), (512, 256), (768, 128), (896, 128 - TWICE), (1024 - TWICE, TWICE))
LAST = len(PASSED) - 1
LEFT = (0, 0, 0, 0, 0, 0, 4, 0), (4, 0, 0, 0, 2, 1, 0, 0)
LATE = 6


def kernel(wg, ag, wu, au, rw_any, gain_any, mix, gate, up, router, held, load_sem, small, small_sem, ring, flat,
           ready, first_recv, second_recv, passed_recv, ici_send, core_sem, r_send, r_recv):
    e, s = lax.axis_index("expert"), lax.axis_index("shard")
    x, y, z_lo = e & (X - 1), (e >> 2) & (Y - 1), e >> 5
    z_hi, c = s >> 1, s & 1
    z = 2 * z_hi + z_lo

    def columns_of(g):
        return pl.ds(GROUPS[g][0] * ROWS, GROUPS[g][1] * ROWS)

    for i, ref in enumerate((rw_any, gain_any)):
        pltpu.make_async_copy(ref, small.at[i], small_sem).start()
    for g in range(len(GROUPS)):
        for k in (1, 0):
            for i, ref in enumerate(((wg, ag), (wu, au))[k]):
                pltpu.make_async_copy(ref.at[0, :, columns_of(g)], held.at[2 * k + i, :, columns_of(g)], load_sem.at[g]).start()

    def loaded(g):
        ref = held.at[:, :, columns_of(g)]
        pltpu.make_async_copy(ref, ref, load_sem.at[g]).wait()

    def place(dx=0, dy=0, dz=0, dc=0):
        return (x + dx) & (X - 1), (y + dy) & (Y - 1), (z + dz) & (Z - 1), (c + dc) & 1

    def device(p):
        return {"expert": ((p[2] & 1) << 5) + (p[1] << 2) + p[0], "shard": (p[2] & 6) + p[3]}

    def rank(p):
        order = (p[2] << 7) + (p[1] << 4) + (p[0] << 2) + 2 - 2 * p[3]
        return jnp.where(order == 2, (LATE << 7) - 1, order)

    places = [place(dz=2), place(dz=-2), place(dc=1), place(dz=1), place(dz=-1), place(dx=1), place(dx=-1), place(dy=1), place(dy=-1),
              place(dz=2, dc=1), place(dz=-2, dc=1)]
    near = [device(p) for p in places]
    own_rank = rank(place())
    earlier = [rank(p) < own_rank for p in places]
    lanes = (FORE, BACK)

    barrier = pltpu.get_barrier_semaphore()
    for k in range(11):
        @pl.when(jnp.logical_not(earlier[k]))
        def _():
            pl.semaphore_signal(barrier, inc=1, device_id=near[k], device_id_type=MESH)
    def answer():
        before = sum(a.astype(jnp.int32) for a in earlier)

        @pl.when(before > 0)
        def _():
            pl.semaphore_wait(barrier, before)

        for k in range(11):
            @pl.when(earlier[k])
            def _():
                pl.semaphore_signal(ready.at[min(OPPOSITE[k], ZP)], inc=1, device_id=near[k], device_id_type=MESH)

    def allow(k):
        @pl.when(jnp.logical_not(earlier[k]))
        def _():
            pl.semaphore_wait(ready.at[k], 1)

    def allow_rest():
        after = sum(1 - earlier[k].astype(jnp.int32) for k in range(ZP, 11))

        @pl.when(after > 0)
        def _():
            pl.semaphore_wait(ready.at[ZP], after)

    share = mix[...]
    rest = 1.0 - share

    def columns(shard):
        return pl.ds(pl.multiple_of(shard * WIDE, WIDE), WIDE)

    def rows(j, n=1):
        return pl.ds(pl.multiple_of(j * ROWS, ROWS), n * ROWS)

    def compute(k, j):
        fresh = share * held[2 * k, :, rows(j)] + rest * held[2 * k + 1, :, rows(j)]
        (gate, up)[k][rows(j), columns(s)] = fresh.T.astype(jnp.bfloat16)

    def copy(k, shard, lo, n, to, send, recv):
        ref = (gate, up)[k].at[pl.ds(lo, n), columns(shard)]
        return pltpu.make_async_remote_copy(ref, ref, send, recv, device_id=near[to], device_id_type=MESH)

    def chunks(j, n):
        return j * ROWS, n * ROWS

    def first(lane, i):
        return copy(lane, s, *chunks(*GROUPS[i]), lanes[lane], ici_send, first_recv.at[i])

    def second(lane, i):
        return copy(1 - lane, s, *chunks(*OTHER[i]), lanes[lane], ici_send, second_recv.at[i])

    def passed(lane, p, shard):
        return copy(lane, shard, *PASSED[p], lanes[lane], ici_send, passed_recv.at[p])

    def shared(lane, i, shard, to):
        return copy(lane, shard, i * STEP, STEP, to, ici_send, passed_recv.at[LAST + 2])

    def across(k, shard, lo, n):
        return copy(k, shard, lo, n, MATE, core_sem.at[0], core_sem.at[1])

    def arrived(n, sem):
        ref = gate.at[0:n, 0 : 2 * WIDE]
        pltpu.make_async_remote_copy(ref, ref, core_sem.at[0], sem, device_id=near[MATE], device_id_type=MESH).wait_recv()

    def arriving(lane, far):
        return ((z_hi + (4 - far if lane == 0 else far)) & 3) * 2 + c

    def sent(ref, sem):
        pltpu.make_async_remote_copy(ref, ref, sem, core_sem.at[1], device_id=near[MATE], device_id_type=MESH).wait_send()

    def post(ref, to, i):
        return pltpu.make_async_remote_copy(
            ref, ref, r_send.at[min(i // 2, 1)], r_recv.at[i], device_id=near[to], device_id_type=MESH)

    def piece(k):
        return ring.at[c, y, x, (z + k) & (Z - 1)]

    def row(k):
        return ring.at[c, y, (x + k) & (X - 1)]

    def plane(k):
        return ring.at[c, (y + k) & (Y - 1)]

    def landed(ref, i):
        post(ref, MATE, i).wait_recv()

    even = (z & 1) == 0
    zeroth = jnp.logical_or(z < 2, z >= 6)

    def in_turn(order, do):
        for lane in range(2):
            @pl.when(zeroth if lane == order else jnp.logical_not(zeroth))
            def _():
                do(lane)

    def own_piece(lane):
        post(piece(0), lanes[lane], 0).start()

    def begin(order, *which):
        in_turn(order, lambda lane: [first(lane, i).start() for i in which])

    def begin_other(order, *which):
        in_turn(order, lambda lane: [second(lane, i).start() for i in which])

    both = jnp.logical_and(even, z >= 6)
    one = jnp.logical_and(even, z < 6)

    with jax.named_scope("first_chunk"):
        answer()
        loaded(0)
        compute(1, 0)
        compute(0, 0)
    with jax.named_scope("admit_first"):
        in_turn(0, lambda lane: allow(lanes[lane]))

        @pl.when(even)
        def _():
            begin(0, 0)

        @pl.when(both)
        def _():
            begin(1, 0)
    with jax.named_scope("compute"):
        def more(j, _):
            for k in (1, 0):
                compute(k, j)
            return 0

        def more_of(g):
            loaded(g)
            lax.fori_loop(GROUPS[g][0], sum(GROUPS[g]), more, 0)

        more_of(1)
        pltpu.make_async_copy(small, small, small_sem).wait()
        ring[c, y, x, z] = small[0] * small[1]
        in_turn(0, own_piece)

        @pl.when(even)
        def _():
            begin(0, 1)

        @pl.when(both)
        def _():
            in_turn(1, own_piece)
            begin(1, 1)

        @pl.when(even)
        def _():
            begin_other(0, 0)

        more_of(2)
    with jax.named_scope("admit_second"):
        in_turn(1, lambda lane: allow(lanes[lane]))

        @pl.when(jnp.logical_not(both))
        def _():
            in_turn(1, own_piece)

        @pl.when(one)
        def _():
            begin(1, 0, 1)

        @pl.when(even)
        def _():
            begin_other(1, 0)
    with jax.named_scope("z_steps"):
        allow_rest()
        post(piece(0), ZP, 1).start()
        post(piece(0), ZM, 1).start()
        landed(ring.at[c, y, x, 0:2], 0)
        post(piece(-2), ZP, 1).start()
        post(piece(2), ZM, 1).start()
        post(piece(-2), FORE, 1).start()
    with jax.named_scope("own"):
        @pl.when(jnp.logical_not(even))
        def _():
            for order in range(2):
                begin(order, 0, 1)
                begin_other(order, 0)

        for order in range(2):
            begin(order, 2)
            begin_other(order, 1)
    with jax.named_scope("mate_own"):
        allow(MATE)
        for k in range(2):
            across(k, s, 0, D_EXPERT).start()

    def at_plane(table):
        return sum(jnp.where(z == k, v, 0) for k, v in enumerate(table) if v) + jnp.where(z < 0, 1, 0)

    left = [at_plane(LEFT[lane]) for lane in range(2)]
    taken = [at_plane([LEFT[lane][(k + 4) % Z] for k in range(Z)]) for lane in range(2)]

    odd = jnp.logical_not(even)

    def own_arrived(i):
        with jax.named_scope(f"half_a{i}"):
            start, length = chunks(*GROUPS[i])
            arrived(length, first_recv.at[i])
            for lane in range(2):
                shard = arriving(lane, 1)
                for j in range(MOST):
                    if start <= j * STEP < start + length:
                        @pl.when(j >= left[lane])
                        def _():
                            shared(lane, j, shard, lanes[lane]).start()
                for p, (lo, n) in enumerate(PASSED):
                    if start <= lo < start + length:
                        if p == LAST:
                            again = copy(lane, shard, lo, n, (FORE_MATE, BACK_MATE)[lane], ici_send, passed_recv.at[LAST + 1])
                            more = z == (7, 3)[lane]

                            @pl.when(jnp.logical_and(more, c == 0))
                            def _():
                                again.start()

                            passed(lane, p, shard).start()

                            @pl.when(jnp.logical_and(more, c == 1))
                            def _():
                                again.start()
                        else:
                            passed(lane, p, shard).start()
                across(lane, shard, start, length).start()

    def other_arrived(i):
        with jax.named_scope(f"half_b{i}"):
            start, length = chunks(*OTHER[i])
            arrived(length, second_recv.at[i])
            for lane in range(2):
                for j in range(MOST):
                    if start <= j * STEP < start + length and max(LEFT[lane]) > j:
                        @pl.when(j < taken[lane])
                        def _():
                            shared(lane, j, arriving(1 - lane, 1), lanes[1 - lane]).start()
            for lane in range(2):
                across(1 - lane, arriving(lane, 1), start, length).start()

    def router_rest():
        with jax.named_scope("router_x1"):
            landed(ring.at[c, y, x, 0:5], 1)
            post(row(0), XP, 2).start()
            post(row(0), XM, 2).start()
        with jax.named_scope("router_x2"):
            landed(ring.at[c, y, 0:2], 2)
            post(row(-1), XP, 3).start()
        with jax.named_scope("router_y1"):
            landed(ring.at[c, y, 0], 3)
            post(plane(0), YP, 4).start()
            post(plane(0), YM, 4).start()
        for i in range(3):
            with jax.named_scope(f"router_y{i + 2}"):
                landed(ring.at[c, 0:2], 4 + i)
                post(plane(-1 - i), YP, 5 + i).start()
                if i < 2:
                    post(plane(1 + i), YM, 5 + i).start()
        with jax.named_scope("router_mate"):
            landed(ring.at[c, 0], 7)
            post(ring.at[c], MATE, 8).start()

    def arrivals():
        own_arrived(0)
        own_arrived(1)
        other_arrived(0)
        own_arrived(2)

    @pl.when(even)
    def _():
        arrivals()
        router_rest()
        other_arrived(1)

    @pl.when(jnp.logical_not(even))
    def _():
        router_rest()
        arrivals()
        other_arrived(1)

    with jax.named_scope("router_end"):
        landed(ring.at[1 - c], 8)

        def lay(i, _):
            yy, xx = i >> 2, i & (X - 1)
            for zz in range(Z):
                for cc in range(2):
                    lo = (2 * (zz // 2) + cc) * WIDE
                    flat[pl.ds((zz % 2) * (Y * X) + i, 1), lo : lo + WIDE] = ring[cc, yy, xx, zz]
            return 0

        lax.fori_loop(0, Y * X, lay, 0)
        router[...] = flat[...].astype(jnp.bfloat16)
    def passed_across(lo, n):
        for lane in range(2):
            across(lane, arriving(lane, 2), lo, n).start()

    with jax.named_scope("shared"):
        arrived(MOST * STEP, passed_recv.at[LAST + 2])
        passed_across(0, MOST * STEP)
    for p, (lo, n) in enumerate(PASSED[:LAST]):
        with jax.named_scope(f"passed{p}"):
            arrived(n, passed_recv.at[p])
            passed_across(lo, n)

    with jax.named_scope("finish"):
        def rows_sent(k):
            shared_rows = STEP * (2 * MOST + sum(LEFT[lane][(k + 4) % Z] - LEFT[lane][k] for lane in range(2)))
            return 4 * D_EXPERT + 2 * (D_EXPERT - MOST * STEP) + shared_rows + TWICE * (k in (3, 7))

        sent(ring.at[c, y, x, 0:7], r_send.at[0])
        sent(held.at[0, 0:168, 0:768], r_send.at[1])
        twice = z == 1

        @pl.when(twice)
        def _():
            sent(gate.at[0 : rows_sent(1) // SHARDS, :], ici_send)

        arrived(TWICE, passed_recv.at[LAST])

        @pl.when(jnp.logical_not(twice))
        def _():
            passed_across(*PASSED[LAST])

        for n in sorted({rows_sent(k) for k in range(Z) if k != 1}):
            @pl.when(at_plane([int(k != 1 and rows_sent(k) == n) for k in range(Z)]) > 0)
            def _():
                sent(gate.at[0 : n // SHARDS, :], ici_send)

        def swapped(ref):
            sent(ref, core_sem.at[0])
            pltpu.make_async_remote_copy(ref, ref, core_sem.at[0], core_sem.at[1], device_id=near[MATE], device_id_type=MESH).wait_recv()

        @pl.when(twice)
        def _():
            arrived(TWICE, passed_recv.at[LAST + 1])
            swapped(gate.at[0 : D_EXPERT - 2 * TWICE // SHARDS, :])

        @pl.when(jnp.logical_not(twice))
        def _():
            swapped(gate)


def store(gate, up, router, gate_out, up_out, router_out, sem):
    copies = [pltpu.make_async_copy(a, b, sem.at[i])
              for i, (a, b) in enumerate(((gate, gate_out), (up, up_out), (router, router_out)))]
    for copy in copies:
        copy.start()
    for copy in copies:
        copy.wait()


def local(w_gate, avg_gate, w_up, avg_up, mix_share, router_weight, router_gain):
    out = jax.ShapeDtypeStruct((D_EXPERT, D_MODEL), jnp.bfloat16)
    outs = (out, out, jax.ShapeDtypeStruct((EXPERTS, D_MODEL), jnp.bfloat16))
    hbm = pl.BlockSpec(memory_space=pltpu.HBM)
    vmem = pl.BlockSpec(memory_space=pltpu.VMEM)
    dma = pltpu.SemaphoreType.DMA
    gathered = pl.pallas_call(
        kernel,
        out_shape=outs,
        in_specs=[hbm] * 6 + [vmem],
        out_specs=(vmem,) * 3,
        scratch_shapes=[
            pltpu.VMEM((4, WIDE, D_EXPERT), jnp.float32),
            dma((len(GROUPS),)),
            pltpu.VMEM((2, 1, WIDE), jnp.float32),
            dma,
            pltpu.VMEM((2, Y, X, Z, 1, WIDE), jnp.float32),
            pltpu.VMEM((EXPERTS, D_MODEL), jnp.float32),
            pltpu.SemaphoreType.REGULAR((4,)),
            dma((len(GROUPS),)),
            dma((len(OTHER),)),
            dma((len(PASSED) + 2,)),
            dma,
            dma((2,)),
            dma((2,)),
            dma((9,)),
        ],
        compiler_params=pltpu.CompilerParams(
            collective_id=0, has_side_effects=True, vmem_limit_bytes=40 * 2**20),
        name="mix_and_gather",
    )(*(pltpu.with_memory_space_constraint(a, pltpu.HBM) for a in (
        w_gate, avg_gate, w_up, avg_up, router_weight.reshape(1, WIDE), router_gain.reshape(1, WIDE))),
      mix_share.reshape(1, 1))
    gate, up, router = pl.pallas_call(
        store,
        out_shape=outs,
        in_specs=[vmem] * 3,
        out_specs=(hbm,) * 3,
        scratch_shapes=[dma((3,))],
        compiler_params=pltpu.CompilerParams(vmem_limit_bytes=2**20),
        name="store",
    )(*gathered)
    return gate[None], up[None], router.T


def solution(mesh):
    return jax.shard_map(
        local,
        mesh=mesh,
        in_specs=(
            P("expert", "shard", None),
            P("expert", "shard", None),
            P("expert", "shard", None),
            P("expert", "shard", None),
            P("expert"),
            P("shard", "expert"),
            P("shard"),
        ),
        out_specs=(P("expert", None, None), P("expert", None, None), P()),
        check_vma=False,
    )
```
